32 devices in a mesh: dp: 4 (over x, y), tp: 8 (over z, core).
Axes of the slice: x: 2, y: 2, z: 4, core: 2. Of those that a mesh axis runs over, the one named last changes fastest.
Arguments:
- hidden: bfloat16 [4, 4096, 1536], P('dp'), parts along dimension 0
- norm_w: bfloat16 [2, 1536], replicated
- w_z: bfloat16 [2, 1536, 3072], P(None, None, 'tp')
- w_x: bfloat16 [2, 1536, 3072], P(None, None, 'tp')
- w_bc: bfloat16 [2, 1536, 256], replicated
- w_dt: bfloat16 [2, 1536, 48], P(None, None, 'tp')
- conv_x: bfloat16 [2, 4, 3072], P(None, None, 'tp')
- conv_bc: bfloat16 [2, 4, 256], replicated
- bias_x: bfloat16 [2, 3072], P(None, 'tp')
- bias_bc: bfloat16 [2, 256], replicated
- dt_bias: float32 [2, 48], P(None, 'tp')
- a_log: float32 [2, 48], P(None, 'tp')
- d_skip: float32 [2, 48], P(None, 'tp')
- gate_w: bfloat16 [2, 3072], P(None, 'tp')
- w_out: bfloat16 [2, 3072, 1536], P(None, 'tp')
Outputs:
- output: bfloat16 [4, 4096, 1536], P('dp'), parts along dimension 0
There are 4 independent parts. The reference program is written for one: setup_inputs(seed, part) draws one part's arguments, and reference() takes and returns one part's arrays. A program takes and returns all parts, laid end to end along the dimension named above; an argument that names none is the same for every part.
All inputs are finite; a program needn't handle non-finite values.
Results may differ from the reference program's by a relative error of at most 0.0138432.
Values sent between devices are 32-bit elements.
A program may use at most 1 GiB of HBM per device.

```python
import math
import jax
import jax.numpy as jnp
from jax import lax

BATCH_ROWS = 1
SEQ_LEN = 4096
D_MODEL = 1536
HEADS = 48
HEAD_DIM = 64
STATE_DIM = 128
LAYERS = 2
CONV_WIDTH = 4
BLOCK_LEN = 256

INNER_WIDTH = HEADS * HEAD_DIM
EPSILON = 1e-5


def setup_inputs(seed: int = 0, part: int = 0) -> dict:
    key_list = jax.random.split(jax.random.key(seed), 16)
    part_key = jax.random.fold_in(jax.random.key(seed + 1), part)
    in_scale = D_MODEL ** -0.5
    hidden = jax.random.normal(part_key, (BATCH_ROWS, SEQ_LEN, D_MODEL), jnp.float32)
    head_scale = jnp.exp(jax.random.uniform(key_list[0], (LAYERS, HEADS), jnp.float32, -1.2, 1.2))
    col_scale = jnp.repeat(head_scale, HEAD_DIM, axis=1)[:, None, :]
    dt_init = jnp.exp(jax.random.uniform(key_list[1], (LAYERS, HEADS), jnp.float32, math.log(0.001), math.log(0.1)))
    return {
        'hidden': hidden.astype(jnp.bfloat16),
        'norm_w': (1.0 + 0.2 * jax.random.normal(key_list[2], (LAYERS, D_MODEL), jnp.float32)).astype(jnp.bfloat16),
        'w_z': (in_scale * jax.random.normal(key_list[3], (LAYERS, D_MODEL, INNER_WIDTH), jnp.float32)).astype(jnp.bfloat16),
        'w_x': (in_scale * col_scale * jax.random.normal(key_list[4], (LAYERS, D_MODEL, INNER_WIDTH), jnp.float32)).astype(jnp.bfloat16),
        'w_bc': (in_scale * jax.random.normal(key_list[5], (LAYERS, D_MODEL, 2 * STATE_DIM), jnp.float32)).astype(jnp.bfloat16),
        'w_dt': (0.5 * in_scale * jax.random.normal(key_list[6], (LAYERS, D_MODEL, HEADS), jnp.float32)).astype(jnp.bfloat16),
        'conv_x': (0.5 * jax.random.normal(key_list[7], (LAYERS, CONV_WIDTH, INNER_WIDTH), jnp.float32)).astype(jnp.bfloat16),
        'conv_bc': (0.5 * jax.random.normal(key_list[8], (LAYERS, CONV_WIDTH, 2 * STATE_DIM), jnp.float32)).astype(jnp.bfloat16),
        'bias_x': (0.3 * jax.random.normal(key_list[9], (LAYERS, INNER_WIDTH), jnp.float32)).astype(jnp.bfloat16),
        'bias_bc': (0.3 * jax.random.normal(key_list[10], (LAYERS, 2 * STATE_DIM), jnp.float32)).astype(jnp.bfloat16),
        'dt_bias': dt_init + jnp.log(-jnp.expm1(-dt_init)),
        'a_log': jnp.log(jax.random.uniform(key_list[11], (LAYERS, HEADS), jnp.float32, 1.0, 16.0)),
        'd_skip': jax.random.uniform(key_list[12], (LAYERS, HEADS), jnp.float32, 0.5, 2.0),
        'gate_w': (1.0 + 0.2 * jax.random.normal(key_list[13], (LAYERS, INNER_WIDTH), jnp.float32)).astype(jnp.bfloat16),
        'w_out': (INNER_WIDTH ** -0.5 * jax.random.normal(key_list[14], (LAYERS, INNER_WIDTH, D_MODEL), jnp.float32)).astype(jnp.bfloat16),
    }


def causal_conv(seq_in, kernel, conv_bias):
    n_steps = seq_in.shape[1]
    padded = jnp.pad(seq_in, ((0, 0), (CONV_WIDTH - 1, 0), (0, 0)))
    conv_sum = conv_bias.astype(jnp.float32)
    for tap_index in range(CONV_WIDTH):
        conv_sum = conv_sum + padded[:, tap_index:tap_index + n_steps, :].astype(jnp.float32) * kernel[tap_index].astype(jnp.float32)
    return conv_sum


def ssd_sequence(seq_in):
    x_heads, dt_val, a_vals, b_in, c_in = seq_in
    n_blocks = SEQ_LEN // BLOCK_LEN
    step_ids = jnp.arange(BLOCK_LEN)
    lower_tri = step_ids[:, None] >= step_ids[None, :]

    def block_step(state, block):
        x_block, dt_block, a_block, b_block, c_block = block
        a_cum = jnp.cumsum(a_block, axis=0)
        seg_sum = a_cum[:, None, :] - a_cum[None, :, :]
        decay_mat = jnp.where(lower_tri[:, :, None], jnp.exp(jnp.minimum(seg_sum, 0.0)), 0.0)
        c_dot_b = jnp.einsum('in,jn->ij', c_block, b_block)
        x_dt = x_block * dt_block[:, :, None]
        y_in = jnp.einsum('ijh,jhp->ihp', decay_mat * c_dot_b[:, :, None], x_dt)
        y_st = jnp.einsum('in,hpn->ihp', c_block, state) * jnp.exp(a_cum)[:, :, None]
        tail_decay = jnp.exp(a_cum[-1][None, :] - a_cum)
        new_state = state * jnp.exp(a_cum[-1])[:, None, None] + jnp.einsum('jn,jhp->hpn', b_block, x_dt * tail_decay[:, :, None])
        return new_state, y_in + y_st

    blocks_in = (
        x_heads.reshape(n_blocks, BLOCK_LEN, HEADS, HEAD_DIM),
        dt_val.reshape(n_blocks, BLOCK_LEN, HEADS),
        a_vals.reshape(n_blocks, BLOCK_LEN, HEADS),
        b_in.reshape(n_blocks, BLOCK_LEN, STATE_DIM),
        c_in.reshape(n_blocks, BLOCK_LEN, STATE_DIM),
    )
    init_state = jnp.zeros((HEADS, HEAD_DIM, STATE_DIM), jnp.float32)
    last_state, y_blocks = lax.scan(block_step, init_state, blocks_in)
    return y_blocks.reshape(SEQ_LEN, HEADS, HEAD_DIM)


def mixer_layer(current, layer_params):
    norm_w, w_z, w_x, w_bc, w_dt, conv_x, conv_bc, bias_x, bias_bc, dt_bias, a_log, d_skip, gate_w, w_out = layer_params
    tokens = BATCH_ROWS * SEQ_LEN
    residual = current.astype(jnp.float32)
    normed = (residual * lax.rsqrt(jnp.mean(residual * residual, axis=-1, keepdims=True) + EPSILON) * norm_w.astype(jnp.float32)).astype(jnp.bfloat16)
    flat_in = normed.reshape(tokens, D_MODEL)
    gate_z = jnp.dot(flat_in, w_z, preferred_element_type=jnp.float32).astype(jnp.bfloat16)
    x_pre = jnp.dot(flat_in, w_x, preferred_element_type=jnp.float32).astype(jnp.bfloat16)
    bc_pre = jnp.dot(flat_in, w_bc, preferred_element_type=jnp.float32).astype(jnp.bfloat16)
    dt_pre = jnp.dot(flat_in, w_dt, preferred_element_type=jnp.float32).astype(jnp.bfloat16)
    x_act = jax.nn.silu(causal_conv(x_pre.reshape(BATCH_ROWS, SEQ_LEN, INNER_WIDTH), conv_x, bias_x))
    bc_act = jax.nn.silu(causal_conv(bc_pre.reshape(BATCH_ROWS, SEQ_LEN, 2 * STATE_DIM), conv_bc, bias_bc))
    dt_val = jax.nn.softplus(dt_pre.astype(jnp.float32).reshape(BATCH_ROWS, SEQ_LEN, HEADS) + dt_bias)
    a_vals = -dt_val * jnp.exp(a_log)
    x_heads = x_act.reshape(BATCH_ROWS, SEQ_LEN, HEADS, HEAD_DIM)
    y_heads = lax.map(ssd_sequence, (x_heads, dt_val, a_vals, bc_act[..., :STATE_DIM], bc_act[..., STATE_DIM:]))
    y_heads = y_heads + d_skip[:, None] * x_heads
    gated_v = y_heads.reshape(BATCH_ROWS, SEQ_LEN, INNER_WIDTH) * jax.nn.silu(gate_z.astype(jnp.float32).reshape(BATCH_ROWS, SEQ_LEN, INNER_WIDTH))
    normed_y = (gated_v * lax.rsqrt(jnp.mean(gated_v * gated_v, axis=-1, keepdims=True) + EPSILON) * gate_w.astype(jnp.float32)).astype(jnp.bfloat16)
    mixed_out = jnp.dot(normed_y.reshape(tokens, INNER_WIDTH), w_out, preferred_element_type=jnp.float32)
    return (residual + mixed_out.reshape(BATCH_ROWS, SEQ_LEN, D_MODEL)).astype(jnp.bfloat16)


def reference(hidden, norm_w, w_z, w_x, w_bc, w_dt, conv_x, conv_bc, bias_x, bias_bc, dt_bias, a_log, d_skip, gate_w, w_out):
    params = (norm_w, w_z, w_x, w_bc, w_dt, conv_x, conv_bc, bias_x, bias_bc, dt_bias, a_log, d_skip, gate_w, w_out)

    def layer_step(current, layer_params):
        return mixer_layer(current, layer_params), None

    final_hidden, unused = lax.scan(layer_step, hidden, params)
    return final_hidden
```

```python
import functools

import jax
import jax.numpy as jnp
from jax import lax
from jax.experimental import pallas as pl
from jax.experimental.pallas import tpu as pltpu
from jax.sharding import PartitionSpec as P

EPSILON = 1e-5
CHUNK = 128
PAIR = 128
HEAD_DIM = 64
HIGHEST = lax.Precision.HIGHEST
F32 = jnp.float32
BF16 = jnp.bfloat16

LAG_B, LAG_H, LAG_M, LAG_O, LAG_T, LAG_F1, LAG_F2 = 3, 4, 6, 8, 10, 12, 13
N_V, N_STAT, N_PAIR, N_HOP, N_TOT = 4, 8, 4, 8, 16


def fdot(a, b):
    return jnp.dot(a, b, precision=HIGHEST, preferred_element_type=F32)


def bdot(a, b):
    return jnp.dot(a, b, preferred_element_type=F32)


def kernel(n_chunks, n_layers, tp, inner_width,
           hid, wz, wx, wbc, wdt, wo, par, out,
           cur, wzv, wxv, wbcv, wdtv, wov, conv_in, state, vbuf, stat,
           obuf, pairbuf, hbuf, rbuf_a, rbuf_b, tbuf, halfbuf,
           hid_sem, w_sem, out_sem,
           stat_send, stat_recv, pair_send, pair_recv, hop_send, hop_recv_a, hop_recv_b,
           tot_send_l, tot_send_r, tot_recv, half_send, half_recv):
    n_items = n_chunks * n_layers
    half = out.shape[1] // 2
    width = wz.shape[-1]
    n_pairs = width // PAIR
    me = lax.axis_index('tp')
    z = me // 2
    core = me % 2
    partner = z * 2 + (1 - core)

    def remote(src, dst, send, recv, device):
        return pltpu.make_async_remote_copy(src_ref=src, dst_ref=dst, send_sem=send, recv_sem=recv, device_id={'tp': device}, device_id_type=pl.DeviceIdType.MESH)

    def on_chip(k):
        return jnp.int32(k * 2) + core

    def chunk_rows(c):
        return pl.ds(pl.multiple_of(c * CHUNK, CHUNK), CHUNK)

    def hid_copy(c, k):
        return pltpu.make_async_copy(hid.at[chunk_rows(c), pl.ds(k * half, half)], cur.at[k, chunk_rows(c), :], hid_sem.at[c, k])

    def w_copies(l):
        return [
            pltpu.make_async_copy(wz.at[l], wzv.at[l], w_sem.at[l, 0]),
            pltpu.make_async_copy(wx.at[l], wxv.at[l], w_sem.at[l, 1]),
            pltpu.make_async_copy(wbc.at[l], wbcv.at[l], w_sem.at[l, 2]),
            pltpu.make_async_copy(wdt.at[l], wdtv.at[l], w_sem.at[l, 3]),
            pltpu.make_async_copy(wo.at[l, :, pl.ds(0, half)], wov.at[l, 0], w_sem.at[l, 4]),
            pltpu.make_async_copy(wo.at[l, :, pl.ds(half, half)], wov.at[l, 1], w_sem.at[l, 5]),
        ]

    def out_copy(c, k):
        return pltpu.make_async_copy(cur.at[k, chunk_rows(c), :], out.at[chunk_rows(c), pl.ds(k * half, half)], out_sem.at[c, k])

    for k in range(2):
        hid_copy(0, k).start()
    for copy in w_copies(0):
        copy.start()

    def start_hid(c, carry):
        for k in range(2):
            hid_copy(c, k).start()
        return carry

    lax.fori_loop(1, n_chunks, start_hid, 0)
    for l in range(1, n_layers):
        for copy in w_copies(l):
            copy.start()

    barrier = pltpu.get_barrier_semaphore()
    for d in range(1, tp):
        pl.semaphore_signal(barrier, inc=1, device_id={'tp': (me + d) % tp}, device_id_type=pl.DeviceIdType.MESH)
    pl.semaphore_wait(barrier, tp - 1)

    row_id = lax.broadcasted_iota(jnp.int32, (CHUNK, CHUNK), 0)
    col_id = lax.broadcasted_iota(jnp.int32, (CHUNK, CHUNK), 1)

    def stat_copy(m, d):
        slot = m % N_STAT
        return remote(stat.at[slot, me], stat.at[slot, me], stat_send.at[slot, d], stat_recv.at[slot, me], (me + d) % tp)

    def stat_arrival(m, d):
        slot = m % N_STAT
        peer = (me + d) % tp
        return remote(stat.at[slot, peer], stat.at[slot, peer], stat_send.at[slot, d], stat_recv.at[slot, peer], peer)

    def pair_copy(m):
        slot = m % N_PAIR
        return remote(obuf.at[slot], pairbuf.at[slot], pair_send.at[slot], pair_recv.at[slot], partner)

    def hop_a(m, device):
        slot = m % N_HOP
        return remote(hbuf.at[slot], rbuf_a.at[slot], hop_send.at[slot], hop_recv_a.at[slot], device)

    def hop_b(m, device):
        slot = m % N_HOP
        return remote(hbuf.at[slot], rbuf_b.at[slot], hop_send.at[slot], hop_recv_b.at[slot], device)

    def tot_left(m, device):
        slot = m % N_TOT
        return remote(tbuf.at[slot], tbuf.at[slot], tot_send_l.at[slot], tot_recv.at[slot], device)

    def tot_right(m, device):
        slot = m % N_TOT
        return remote(tbuf.at[slot], tbuf.at[slot], tot_send_r.at[slot], tot_recv.at[slot], device)

    def half_copy(m):
        return remote(tbuf.at[m % N_TOT], halfbuf.at[m % N_PAIR], half_send.at[m % N_PAIR], half_recv.at[m % N_PAIR], partner)

    def stage_a(m):
        l = m // n_chunks
        c = m % n_chunks

        @pl.when(l == 0)
        def _():
            for k in range(2):
                hid_copy(c, k).wait()

        @pl.when(c == 0)
        def _():
            for copy in w_copies(l):
                copy.wait()
            conv_in[0:8, :] = jnp.zeros((8, conv_in.shape[1]), F32)
            state[...] = jnp.zeros_like(state)

        rows = chunk_rows(c)
        u = jnp.concatenate([cur[0, rows, :], cur[1, rows, :]], axis=1).astype(F32)
        scale = lax.rsqrt(jnp.mean(u * u, axis=-1, keepdims=True) + EPSILON)
        h = (u * scale * par[l, 0:1, :]).astype(BF16)
        gate_z = bdot(h, wzv[l]).astype(BF16).astype(F32)
        conv_in[8:8 + CHUNK, 0:width] = bdot(h, wxv[l]).astype(BF16).astype(F32)
        conv_in[8:8 + CHUNK, width:] = bdot(h, wbcv[l]).astype(BF16).astype(F32)
        dt_pre = bdot(h, wdtv[l]).astype(BF16).astype(F32)

        cw = conv_in.shape[1]
        conv = par[l, 5:6, 0:cw]
        for j in range(4):
            conv = conv + conv_in[5 + j:5 + j + CHUNK, :] * par[l, 1 + j:2 + j, 0:cw]
        act = conv * jax.nn.sigmoid(conv)
        conv_in[0:8, :] = conv_in[CHUNK:CHUNK + 8, :]
        n_state = (cw - width) // 2
        b_in = act[:, width:width + n_state]
        c_in = act[:, width + n_state:]

        pre = dt_pre + par[l, 6:7, 0:PAIR]
        dt = jnp.maximum(pre, 0.0) + jnp.log1p(jnp.exp(-jnp.abs(pre)))
        a = -dt * jnp.exp(par[l, 7:8, 0:PAIR])
        lower = row_id >= col_id
        a_cum = fdot(jnp.where(lower, 1.0, 0.0).astype(F32), a)
        a_cum_t = a_cum.T
        a_last = a_cum[CHUNK - 1:CHUNK, :]
        grow = jnp.exp(a_cum)
        tail = jnp.exp(a_last - a_cum)
        carry = jnp.exp(a_last)
        c_dot_b = lax.dot_general(c_in, b_in, (((1,), (1,)), ((), ())), precision=HIGHEST, preferred_element_type=F32)
        b_t = b_in.T
        first = lax.broadcasted_iota(jnp.int32, (1, PAIR), 1) < HEAD_DIM
        v_slot = m % N_V
        sq = jnp.zeros((CHUNK, PAIR), F32)
        for p in range(n_pairs):
            lanes = slice(p * PAIR, (p + 1) * PAIR)

            def spread(q):
                return jnp.where(first, q[:, 2 * p:2 * p + 1], q[:, 2 * p + 1:2 * p + 2])

            def mix(n):
                seg = a_cum[:, n:n + 1] - a_cum_t[n:n + 1, :]
                return jnp.where(lower, jnp.exp(jnp.minimum(seg, 0.0)), 0.0) * c_dot_b

            x = act[:, lanes]
            x_dt = x * spread(dt)
            y_in = jnp.where(first, fdot(mix(2 * p), x_dt), fdot(mix(2 * p + 1), x_dt))
            s_in = state[:, lanes]
            y_st = fdot(c_in, s_in) * spread(grow)
            state[:, lanes] = s_in * spread(carry) + fdot(b_t, x_dt * spread(tail))
            y = y_in + y_st + par[l, 8:9, lanes] * x
            zp = gate_z[:, lanes]
            v = y * (zp * jax.nn.sigmoid(zp))
            vbuf[v_slot, :, lanes] = v
            sq = sq + v * v
        part = jnp.broadcast_to(jnp.sum(sq, axis=-1, keepdims=True), (CHUNK, PAIR)).T
        stat[m % N_STAT, me] = part[0:8, :]
        for d in range(1, tp):
            stat_copy(m, d).start()

    def stage_b(m):
        l = m // n_chunks
        for d in range(1, tp):
            stat_copy(m, d).wait_send()
            stat_arrival(m, d).wait_recv()
        slot = m % N_STAT
        total = stat[slot, 0]
        for s in range(1, tp):
            total = total + stat[slot, s]
        total = jnp.broadcast_to(total[0:1, :], (PAIR, CHUNK)).T
        scale = lax.rsqrt(total / inner_width + EPSILON)
        parts = []
        for p in range(n_pairs):
            lanes = slice(p * PAIR, (p + 1) * PAIR)
            parts.append((vbuf[m % N_V, :, lanes] * scale * par[l, 9:10, lanes]).astype(BF16))
        g = jnp.concatenate(parts, axis=1)
        obuf[m % N_PAIR] = bdot(g, wov[l, 1 - core])
        pair_copy(m).start()
        hbuf[m % N_HOP] = bdot(g, wov[l, core])

    def stage_h(m):
        pair_copy(m).wait()
        slot = m % N_HOP
        hbuf[slot] = hbuf[slot] + pairbuf[m % N_PAIR]

        @pl.when(z == 0)
        def _():
            hop_a(m, on_chip(1)).start()

        @pl.when(z == 3)
        def _():
            hop_a(m, on_chip(2)).start()

    def stage_m(m):
        @pl.when(z == 2)
        def _():
            hop_a(m, on_chip(3)).wait_recv()
            slot = m % N_HOP
            hbuf[slot] = hbuf[slot] + rbuf_a[slot]
            hop_b(m, on_chip(1)).start()

    def stage_o(m):
        @pl.when(z == 1)
        def _():
            hop_a(m, on_chip(0)).wait_recv()
            hop_b(m, on_chip(2)).wait_recv()
            slot = m % N_HOP
            tbuf[m % N_TOT] = rbuf_a[slot] + hbuf[slot] + rbuf_b[slot]
            tot_left(m, on_chip(0)).start()
            tot_right(m, on_chip(2)).start()

    def stage_t(m):
        @pl.when(z == 0)
        def _():
            hop_a(m, on_chip(1)).wait_send()
            tot_left(m, on_chip(1)).wait_recv()

        @pl.when(z == 1)
        def _():
            tot_left(m, on_chip(0)).wait_send()
            tot_right(m, on_chip(2)).wait_send()

        @pl.when(z == 2)
        def _():
            hop_b(m, on_chip(1)).wait_send()
            tot_right(m, on_chip(1)).wait_recv()
            tot_right(m, on_chip(3)).start()

        @pl.when(z == 3)
        def _():
            hop_a(m, on_chip(2)).wait_send()

    def stage_f1(m):
        @pl.when(z == 2)
        def _():
            tot_right(m, on_chip(3)).wait_send()

        @pl.when(z == 3)
        def _():
            tot_right(m, on_chip(2)).wait_recv()

        half_copy(m).start()

    def stage_f2(m):
        l = m // n_chunks
        c = m % n_chunks
        half_copy(m).wait()
        rows = chunk_rows(c)
        cur[core, rows, :] = (cur[core, rows, :].astype(F32) + tbuf[m % N_TOT]).astype(BF16)
        cur[1 - core, rows, :] = (cur[1 - core, rows, :].astype(F32) + halfbuf[m % N_PAIR]).astype(BF16)

        @pl.when(l == n_layers - 1)
        def _():
            for k in range(2):
                out_copy(c, k).start()

    def step(i, carry):
        for lag, stage in ((LAG_F2, stage_f2), (LAG_F1, stage_f1), (LAG_T, stage_t), (LAG_O, stage_o), (LAG_M, stage_m), (LAG_H, stage_h), (LAG_B, stage_b), (0, stage_a)):
            item = i - lag

            @pl.when(jnp.logical_and(item >= 0, item < n_items))
            def _(item=item, stage=stage):
                stage(item)
        return carry

    lax.fori_loop(0, n_items + LAG_F2, step, 0)

    def end_out(c, carry):
        for k in range(2):
            out_copy(c, k).wait()
        return carry

    lax.fori_loop(0, n_chunks, end_out, 0)


def solution(mesh):
    tp = mesh.shape['tp']
    rep_spec = P()
    col_spec = P(None, None, 'tp')
    vec_spec = P(None, 'tp')
    in_specs = (P('dp'), rep_spec, col_spec, col_spec, rep_spec, col_spec, col_spec, rep_spec, vec_spec, rep_spec, vec_spec, vec_spec, vec_spec, vec_spec, P(None, 'tp', None))

    def device_forward(hidden, norm_w, w_z, w_x, w_bc, w_dt, conv_x, conv_bc, bias_x, bias_bc, dt_bias, a_log, d_skip, gate_w, w_out):
        n_layers, d_model, width = w_z.shape
        n_steps = hidden.shape[1]
        n_chunks = n_steps // CHUNK
        bc_width = w_bc.shape[-1]
        heads = dt_bias.shape[-1]
        half = d_model // 2

        def line(v):
            v = v.astype(F32)
            v = v if v.ndim == 3 else v[:, None, :]
            return jnp.pad(v, ((0, 0), (0, 0), (0, d_model - v.shape[-1])))

        par = jnp.concatenate([
            line(norm_w),
            line(jnp.concatenate([conv_x, conv_bc], axis=-1)),
            line(jnp.concatenate([bias_x, bias_bc], axis=-1)),
            line(dt_bias), line(a_log), line(jnp.repeat(d_skip, HEAD_DIM, axis=-1)), line(gate_w),
        ], axis=1)
        w_dt = jnp.pad(w_dt, ((0, 0), (0, 0), (0, PAIR - heads)))

        any_spec = pl.BlockSpec(memory_space=pl.ANY)
        dma = pltpu.SemaphoreType.DMA
        block = (CHUNK, half)
        out = pl.pallas_call(
            functools.partial(kernel, n_chunks, n_layers, tp, width * tp),
            out_shape=jax.ShapeDtypeStruct((n_steps, d_model), BF16),
            in_specs=[any_spec] * 6 + [pl.BlockSpec(memory_space=pltpu.VMEM)],
            out_specs=any_spec,
            scratch_shapes=[
                pltpu.VMEM((2, n_steps, half), BF16),
                pltpu.VMEM((n_layers, d_model, width), BF16),
                pltpu.VMEM((n_layers, d_model, width), BF16),
                pltpu.VMEM((n_layers, d_model, bc_width), BF16),
                pltpu.VMEM((n_layers, d_model, PAIR), BF16),
                pltpu.VMEM((n_layers, 2, width, half), BF16),
                pltpu.VMEM((CHUNK + 8, width + bc_width), F32),
                pltpu.VMEM((bc_width // 2, width), F32),
                pltpu.VMEM((N_V, CHUNK, width), F32),
                pltpu.VMEM((N_STAT, tp, 8, CHUNK), F32),
                pltpu.VMEM((N_PAIR,) + block, F32),
                pltpu.VMEM((N_PAIR,) + block, F32),
                pltpu.VMEM((N_HOP,) + block, F32),
                pltpu.VMEM((N_HOP,) + block, F32),
                pltpu.VMEM((N_HOP,) + block, F32),
                pltpu.VMEM((N_TOT,) + block, F32),
                pltpu.VMEM((N_PAIR,) + block, F32),
                dma((n_chunks, 2)), dma((n_layers, 6)), dma((n_chunks, 2)),
                dma((N_STAT, tp)), dma((N_STAT, tp)), dma((N_PAIR,)), dma((N_PAIR,)),
                dma((N_HOP,)), dma((N_HOP,)), dma((N_HOP,)),
                dma((N_TOT,)), dma((N_TOT,)), dma((N_TOT,)), dma((N_PAIR,)), dma((N_PAIR,)),
            ],
            compiler_params=pltpu.CompilerParams(collective_id=0, has_side_effects=True, vmem_limit_bytes=60 * 1024 * 1024),
        )(hidden.reshape(n_steps, d_model), w_z, w_x, w_bc, w_dt, w_out, par)
        return out.reshape(1, n_steps, d_model)

    return jax.shard_map(device_forward, mesh=mesh, in_specs=in_specs, out_specs=P('dp'), check_vma=False)
```

```python
import functools

import jax
import jax.numpy as jnp
from jax import lax
from jax.experimental import pallas as pl
from jax.experimental.pallas import tpu as pltpu
from jax.sharding import PartitionSpec as P

EPSILON = 1e-5
CHUNK = 128
PAIR = 128
HEAD_DIM = 64
HIGHEST = lax.Precision.HIGHEST
F32 = jnp.float32
BF16 = jnp.bfloat16

LAG_B, LAG_H, LAG_M, LAG_O, LAG_T, LAG_F1, LAG_F2 = 3, 4, 6, 8, 10, 12, 13
N_V, N_STAT, N_PAIR, N_HOP, N_TOT = 4, 8, 4, 8, 16
EARLY_TWO, EARLY_ONE = 2, 5
SUB = 4
SUB_ROWS = CHUNK // SUB
AHEAD = 4
VMEM_BYTES = 67043328
ROW_CONV, ROW_BIAS, ROW_NORM, ROW_GATE, ROW_SKIP, ROW_DT, ROW_A = 0, 4, 5, 6, 7, 8, 9


def fdot(a, b):
    return jnp.dot(a, b, precision=HIGHEST, preferred_element_type=F32)


def bdot(a, b):
    return jnp.dot(a, b, preferred_element_type=F32)


def kernel(n_chunks, n_layers, tp, inner_width,
           hid, wz, wx, wbc, wo, small_0, small_1, small_2, small_3, small_4, small_5, small_6, small_7, small_8, small_9, cur,
           wzv, wxv, wbcv, wdtv, dt_rows, wov, par, conv_in, state, vbuf, stat,
           obuf, pairbuf, hbuf, rbuf_a, rbuf_b, tbuf, halfbuf,
           norm_w, wdt, conv_x, conv_bc, bias_x, bias_bc, dt_bias, a_log, d_skip, gate_w,
           hid_sem, w_sem, small_sem,
           stat_send, stat_recv, pair_send, pair_recv, hop_send, hop_recv_a, hop_recv_b,
           tot_send_l, tot_send_r, tot_recv, half_send, half_recv):
    n_items = n_chunks * n_layers
    half = cur.shape[1] // 2
    width = wz.shape[-1]
    bc_width = wbc.shape[-1]
    heads = dt_bias.shape[-1]
    n_pairs = width // PAIR
    n_chips = tp // 2
    me = lax.axis_index('tp')
    z = me // 2
    core = me % 2
    partner = z * 2 + (1 - core)
    role = z + core * (n_chips - 1 - 2 * z)

    def on_line(k):
        return (k + core * (n_chips - 1 - 2 * k)) * 2 + core

    def remote(src, dst, send, recv, device):
        return pltpu.make_async_remote_copy(src_ref=src, dst_ref=dst, send_sem=send, recv_sem=recv, device_id={'tp': device}, device_id_type=pl.DeviceIdType.MESH)

    def chunk_rows(c):
        return pl.ds(pl.multiple_of(c * CHUNK, CHUNK), CHUNK)

    def hid_copy(c):
        return pltpu.make_async_copy(hid.at[chunk_rows(c), :], cur.at[chunk_rows(c), :], hid_sem.at[c])

    def w_copies(l):
        return [
            pltpu.make_async_copy(wz.at[l], wzv.at[l], w_sem.at[l, 0]),
            pltpu.make_async_copy(wx.at[l], wxv.at[l], w_sem.at[l, 1]),
            pltpu.make_async_copy(wbc.at[l], wbcv.at[l], w_sem.at[l, 2]),
            pltpu.make_async_copy(wo.at[l, :, pl.ds(0, half)], wov.at[l, 0], w_sem.at[l, 3]),
            pltpu.make_async_copy(wo.at[l, :, pl.ds(half, half)], wov.at[l, 1], w_sem.at[l, 4]),
        ]

    sources = (small_0, small_1, small_2, small_3, small_4, small_5, small_6, small_7, small_8, small_9)
    small = [pltpu.make_async_copy(src, dst, small_sem.at[k]) for k, (src, dst) in enumerate(zip(sources, (norm_w, wdt, conv_x, conv_bc, bias_x, bias_bc, dt_bias, a_log, d_skip, gate_w)))]
    for copy in small:
        copy.start()
    hid_copy(0).start()
    for copy in w_copies(0):
        copy.start()
    for c in range(1, AHEAD):
        hid_copy(c).start()

    barrier = pltpu.get_barrier_semaphore()
    for d in range(1, tp):
        pl.semaphore_signal(barrier, inc=1, device_id={'tp': (me + d) % tp}, device_id_type=pl.DeviceIdType.MESH)

    par[...] = jnp.zeros_like(par)
    dt_rows[...] = jnp.zeros_like(dt_rows)
    wdtv[...] = jnp.zeros_like(wdtv)
    for copy in small:
        copy.wait()
    for l in range(n_layers):
        par[l, ROW_CONV:ROW_CONV + 4, 0:width] = conv_x[l].astype(F32)
        par[l, ROW_CONV:ROW_CONV + 4, width:width + bc_width] = conv_bc[l].astype(F32)
        par[l, ROW_BIAS:ROW_BIAS + 1, 0:width] = bias_x[...].astype(F32)[l:l + 1]
        par[l, ROW_BIAS:ROW_BIAS + 1, width:width + bc_width] = bias_bc[...].astype(F32)[l:l + 1]
        par[l, ROW_NORM:ROW_NORM + 1, :] = norm_w[...].astype(F32)[l:l + 1]
        par[l, ROW_GATE:ROW_GATE + 1, 0:width] = gate_w[...].astype(F32)[l:l + 1]
        par[l, ROW_SKIP:ROW_SKIP + 1, 0:heads] = d_skip[l:l + 1, :]
        par[l, ROW_DT:ROW_DT + 1, 0:heads] = dt_bias[l:l + 1, :]
        par[l, ROW_A:ROW_A + 1, 0:heads] = a_log[l:l + 1, :]
        for n in range(heads):
            dt_rows[n:n + 1, :] = wdt[n].astype(F32)[l:l + 1]
        wdtv[l, 0:dt_rows.shape[0], :] = dt_rows[...].astype(BF16)
    pl.semaphore_wait(barrier, tp - 1)

    row_id = lax.broadcasted_iota(jnp.int32, (CHUNK, CHUNK), 0)
    col_id = lax.broadcasted_iota(jnp.int32, (CHUNK, CHUNK), 1)

    def stat_copy(m, d):
        slot = m % N_STAT
        return remote(stat.at[slot, me], stat.at[slot, me], stat_send.at[slot, d], stat_recv.at[slot, me], (me + d) % tp)

    def stat_arrival(m, d):
        slot = m % N_STAT
        peer = (me + d) % tp
        return remote(stat.at[slot, peer], stat.at[slot, peer], stat_send.at[slot, d], stat_recv.at[slot, peer], peer)

    def pair_copy(m):
        slot = m % N_PAIR
        return remote(obuf.at[slot], pairbuf.at[slot], pair_send.at[slot], pair_recv.at[slot], partner)

    def sub(s):
        return pl.ds(s * SUB_ROWS, SUB_ROWS)

    def hop_a(m, s, device):
        slot = m % N_HOP
        return remote(hbuf.at[slot, sub(s)], rbuf_a.at[slot, sub(s)], hop_send.at[slot, s], hop_recv_a.at[slot, s], device)

    def hop_b(m, s, device):
        slot = m % N_HOP
        return remote(hbuf.at[slot, sub(s)], rbuf_b.at[slot, sub(s)], hop_send.at[slot, s], hop_recv_b.at[slot, s], device)

    def tot_back(m, s, device):
        slot = m % N_TOT
        return remote(tbuf.at[slot, sub(s)], tbuf.at[slot, sub(s)], tot_send_l.at[slot, s], tot_recv.at[slot, s], device)

    def tot_on(m, s, device):
        slot = m % N_TOT
        return remote(tbuf.at[slot, sub(s)], tbuf.at[slot, sub(s)], tot_send_r.at[slot, s], tot_recv.at[slot, s], device)

    def half_copy(m, s):
        slot = m % N_PAIR
        return remote(tbuf.at[m % N_TOT, sub(s)], halfbuf.at[slot, sub(s)], half_send.at[slot, s], half_recv.at[slot, s], partner)

    def stage_a(m):
        l = m // n_chunks
        c = m % n_chunks

        @pl.when(l == 0)
        def _():
            hid_copy(c).wait()

        @pl.when(m + AHEAD < n_chunks)
        def _():
            hid_copy(m + AHEAD).start()

        for later in range(1, n_layers):
            @pl.when(m == later * AHEAD)
            def _(later=later):
                for copy in w_copies(later):
                    copy.start()

        @pl.when(c == 0)
        def _():
            for copy in w_copies(l):
                copy.wait()
            conv_in[0:8, :] = jnp.zeros((8, conv_in.shape[1]), F32)
            state[...] = jnp.zeros_like(state)

        rows = chunk_rows(c)
        u = cur[rows, :].astype(F32)
        scale = lax.rsqrt(jnp.mean(u * u, axis=-1, keepdims=True) + EPSILON)
        h = (u * scale * par[l, ROW_NORM:ROW_NORM + 1, :]).astype(BF16)
        gate_z = bdot(h, wzv[l]).astype(BF16).astype(F32)
        conv_in[8:8 + CHUNK, 0:width] = bdot(h, wxv[l]).astype(BF16).astype(F32)
        conv_in[8:8 + CHUNK, width:] = bdot(h, wbcv[l]).astype(BF16).astype(F32)
        dt_pre = lax.dot_general(h, wdtv[l], (((1,), (1,)), ((), ())), preferred_element_type=F32).astype(BF16).astype(F32)

        cw = conv_in.shape[1]
        conv = par[l, ROW_BIAS:ROW_BIAS + 1, 0:cw]
        for j in range(4):
            conv = conv + conv_in[5 + j:5 + j + CHUNK, :] * par[l, ROW_CONV + j:ROW_CONV + j + 1, 0:cw]
        act = conv * jax.nn.sigmoid(conv)
        conv_in[0:8, :] = conv_in[CHUNK:CHUNK + 8, :]
        n_state = (cw - width) // 2
        b_in = act[:, width:width + n_state]
        c_in = act[:, width + n_state:]

        pre = dt_pre + par[l, ROW_DT:ROW_DT + 1, 0:PAIR]
        dt = jnp.maximum(pre, 0.0) + jnp.log1p(jnp.exp(-jnp.abs(pre)))
        a = -dt * jnp.exp(par[l, ROW_A:ROW_A + 1, 0:PAIR])
        lower = row_id >= col_id
        a_cum = fdot(jnp.where(lower, 1.0, 0.0).astype(F32), a)
        a_cum_t = a_cum.T
        a_last = a_cum[CHUNK - 1:CHUNK, :]
        grow = jnp.exp(a_cum)
        tail = jnp.exp(a_last - a_cum)
        carry = jnp.exp(a_last)
        c_dot_b = lax.dot_general(c_in, b_in, (((1,), (1,)), ((), ())), precision=HIGHEST, preferred_element_type=F32)
        b_t = b_in.T
        first = lax.broadcasted_iota(jnp.int32, (1, PAIR), 1) < HEAD_DIM
        v_slot = m % N_V
        sq = jnp.zeros((CHUNK, PAIR), F32)
        skip = par[l, ROW_SKIP:ROW_SKIP + 1, 0:PAIR]
        for p in range(n_pairs):
            lanes = slice(p * PAIR, (p + 1) * PAIR)

            def spread(q):
                return jnp.where(first, q[:, 2 * p:2 * p + 1], q[:, 2 * p + 1:2 * p + 2])

            def mix(n):
                seg = a_cum[:, n:n + 1] - a_cum_t[n:n + 1, :]
                return jnp.where(lower, jnp.exp(jnp.minimum(seg, 0.0)), 0.0) * c_dot_b

            x = act[:, lanes]
            x_dt = x * spread(dt)
            y_in = jnp.where(first, fdot(mix(2 * p), x_dt), fdot(mix(2 * p + 1), x_dt))
            s_in = state[:, lanes]
            y_st = fdot(c_in, s_in) * spread(grow)
            state[:, lanes] = s_in * spread(carry) + fdot(b_t, x_dt * spread(tail))
            y = y_in + y_st + spread(skip) * x
            zp = gate_z[:, lanes]
            v = y * (zp * jax.nn.sigmoid(zp))
            vbuf[v_slot, :, lanes] = v
            sq = sq + v * v
        part = jnp.broadcast_to(jnp.sum(sq, axis=-1, keepdims=True), (CHUNK, PAIR)).T
        stat[m % N_STAT, me] = part[0:8, :]
        for d in range(1, tp):
            stat_copy(m, d).start()

    def stage_b(m):
        l = m // n_chunks
        for d in range(1, tp):
            stat_copy(m, d).wait_send()
            stat_arrival(m, d).wait_recv()
        slot = m % N_STAT
        total = stat[slot, 0]
        for s in range(1, tp):
            total = total + stat[slot, s]
        total = jnp.broadcast_to(total[0:1, :], (PAIR, CHUNK)).T
        scale = lax.rsqrt(total / inner_width + EPSILON)
        parts = []
        for p in range(n_pairs):
            lanes = slice(p * PAIR, (p + 1) * PAIR)
            parts.append((vbuf[m % N_V, :, lanes] * scale * par[l, ROW_GATE:ROW_GATE + 1, lanes]).astype(BF16))
        g = jnp.concatenate(parts, axis=1)
        obuf[m % N_PAIR] = bdot(g, wov[l, 1 - core])
        pair_copy(m).start()
        hbuf[m % N_HOP] = bdot(g, wov[l, core])

    def stage_h(m):
        pair_copy(m).wait()
        slot = m % N_HOP
        hbuf[slot] = hbuf[slot] + pairbuf[m % N_PAIR]

        @pl.when(role == 0)
        def _():
            for s in range(SUB):
                hop_a(m, s, on_line(1)).start()

        @pl.when(role == 3)
        def _():
            for s in range(SUB):
                hop_a(m, s, on_line(2)).start()

    def stage_m(m):
        @pl.when(role == 2)
        def _():
            slot = m % N_HOP
            for s in range(SUB):
                hop_a(m, s, on_line(3)).wait_recv()
                hbuf[slot, sub(s)] = hbuf[slot, sub(s)] + rbuf_a[slot, sub(s)]
                hop_b(m, s, on_line(1)).start()

    def stage_o(m):
        @pl.when(role == 1)
        def _():
            slot = m % N_HOP
            for s in range(SUB):
                hop_a(m, s, on_line(0)).wait_recv()
                hop_b(m, s, on_line(2)).wait_recv()
                tbuf[m % N_TOT, sub(s)] = rbuf_a[slot, sub(s)] + hbuf[slot, sub(s)] + rbuf_b[slot, sub(s)]
                tot_on(m, s, on_line(2)).start()
                tot_back(m, s, on_line(0)).start()

    def stage_t(m):
        @pl.when(role == 0)
        def _():
            for s in range(SUB):
                hop_a(m, s, on_line(1)).wait_send()
                tot_back(m, s, on_line(1)).wait_recv()

        @pl.when(role == 1)
        def _():
            for s in range(SUB):
                tot_back(m, s, on_line(0)).wait_send()
                tot_on(m, s, on_line(2)).wait_send()

        @pl.when(role == 2)
        def _():
            for s in range(SUB):
                hop_b(m, s, on_line(1)).wait_send()
                tot_on(m, s, on_line(1)).wait_recv()
                tot_on(m, s, on_line(3)).start()

        @pl.when(role == 3)
        def _():
            for s in range(SUB):
                hop_a(m, s, on_line(2)).wait_send()

    def stage_f1(m):
        for s in range(SUB):
            @pl.when(role == 3)
            def _(s=s):
                tot_on(m, s, on_line(2)).wait_recv()

            half_copy(m, s).start()

    def stage_f2(m):
        @pl.when(role == 2)
        def _():
            for s in range(SUB):
                tot_on(m, s, on_line(3)).wait_send()

        own = pl.ds(pl.multiple_of(core * half, PAIR), half)
        other = pl.ds(pl.multiple_of((1 - core) * half, PAIR), half)
        for s in range(SUB):
            half_copy(m, s).wait()
            rows = pl.ds(pl.multiple_of((m % n_chunks) * CHUNK + s * SUB_ROWS, SUB_ROWS), SUB_ROWS)
            cur[rows, own] = (cur[rows, own].astype(F32) + tbuf[m % N_TOT, sub(s)]).astype(BF16)
            cur[rows, other] = (cur[rows, other].astype(F32) + halfbuf[m % N_PAIR, sub(s)]).astype(BF16)

    def step(i, carry):
        for lag, stage in ((LAG_F2, stage_f2), (LAG_F1, stage_f1), (LAG_T, stage_t), (LAG_O, stage_o), (LAG_M, stage_m), (LAG_H, stage_h), (LAG_B, stage_b)):
            k = i - lag
            item = jnp.where(k >= EARLY_ONE, k, jnp.where(k >= EARLY_TWO - 1, k + 1, k + 2))
            steady = jnp.logical_and(k >= EARLY_ONE, k < n_items)
            one_early = jnp.logical_and(k + 1 >= EARLY_TWO, k + 1 < EARLY_ONE)
            two_early = jnp.logical_and(k + 2 >= 0, k + 2 < EARLY_TWO)

            @pl.when(jnp.logical_or(steady, jnp.logical_or(one_early, two_early)))
            def _(item=item, stage=stage):
                stage(item)

        @pl.when(i < n_items)
        def _():
            stage_a(i)
        return carry

    lax.fori_loop(0, n_items + LAG_F2, step, 0)


def write_out(cur, out, sem):
    n_parts = sem.shape[0]
    rows = cur.shape[0] // n_parts
    copies = [pltpu.make_async_copy(cur.at[pl.ds(k * rows, rows)], out.at[pl.ds(k * rows, rows)], sem.at[k]) for k in range(n_parts)]
    for copy in copies:
        copy.start()
    for copy in copies:
        copy.wait()


def solution(mesh):
    tp = mesh.shape['tp']
    rep_spec = P()
    col_spec = P(None, None, 'tp')
    vec_spec = P(None, 'tp')
    in_specs = (P('dp'), rep_spec, col_spec, col_spec, rep_spec, col_spec, col_spec, rep_spec, vec_spec, rep_spec, vec_spec, vec_spec, vec_spec, vec_spec, P(None, 'tp', None))

    def device_forward(hidden, norm_w, w_z, w_x, w_bc, w_dt, conv_x, conv_bc, bias_x, bias_bc, dt_bias, a_log, d_skip, gate_w, w_out):
        n_layers, d_model, width = w_z.shape
        n_steps = hidden.shape[1]
        n_chunks = n_steps // CHUNK
        bc_width = w_bc.shape[-1]
        half = d_model // 2
        small = (norm_w, jnp.transpose(w_dt, (2, 0, 1)), conv_x, conv_bc, bias_x, bias_bc, dt_bias, a_log, d_skip, gate_w)
        hbm_spec = pl.BlockSpec(memory_space=pltpu.HBM)
        vmem_spec = pl.BlockSpec(memory_space=pltpu.VMEM)
        dma = pltpu.SemaphoreType.DMA
        block = (CHUNK, half)
        out = pl.pallas_call(
            functools.partial(kernel, n_chunks, n_layers, tp, width * tp),
            out_shape=pltpu.VMEM((n_steps, d_model), BF16),
            in_specs=[hbm_spec] * (5 + len(small)),
            out_specs=vmem_spec,
            scratch_shapes=[
                pltpu.VMEM((n_layers, d_model, width), BF16),
                pltpu.VMEM((n_layers, d_model, width), BF16),
                pltpu.VMEM((n_layers, d_model, bc_width), BF16),
                pltpu.VMEM((n_layers, PAIR, d_model), BF16),
                pltpu.VMEM((16, d_model), F32),
                pltpu.VMEM((n_layers, 2, width, half), BF16),
                pltpu.VMEM((n_layers, 16, d_model), F32),
                pltpu.VMEM((CHUNK + 8, width + bc_width), F32),
                pltpu.VMEM((bc_width // 2, width), F32),
                pltpu.VMEM((N_V, CHUNK, width), F32),
                pltpu.VMEM((N_STAT, tp, 8, CHUNK), F32),
                pltpu.VMEM((N_PAIR,) + block, F32),
                pltpu.VMEM((N_PAIR,) + block, F32),
                pltpu.VMEM((N_HOP,) + block, F32),
                pltpu.VMEM((N_HOP,) + block, F32),
                pltpu.VMEM((N_HOP,) + block, F32),
                pltpu.VMEM((N_TOT,) + block, F32),
                pltpu.VMEM((N_PAIR,) + block, F32),
                *[pltpu.VMEM(v.shape, v.dtype) for v in small],
                dma((n_chunks,)), dma((n_layers, 5)), dma((len(small),)),
                dma((N_STAT, tp)), dma((N_STAT, tp)), dma((N_PAIR,)), dma((N_PAIR,)),
                dma((N_HOP, SUB)), dma((N_HOP, SUB)), dma((N_HOP, SUB)),
                dma((N_TOT, SUB)), dma((N_TOT, SUB)), dma((N_TOT, SUB)), dma((N_PAIR, SUB)), dma((N_PAIR, SUB)),
            ],
            compiler_params=pltpu.CompilerParams(collective_id=0, has_side_effects=True, vmem_limit_bytes=VMEM_BYTES - 2 * n_steps * d_model),
        )(hidden.reshape(n_steps, d_model), w_z, w_x, w_bc, w_out, *small)
        out = pl.pallas_call(
            write_out,
            out_shape=jax.ShapeDtypeStruct((n_steps, d_model), BF16),
            in_specs=[vmem_spec],
            out_specs=hbm_spec,
            scratch_shapes=[dma((8,))],
            compiler_params=pltpu.CompilerParams(vmem_limit_bytes=1024 * 1024),
        )(out)
        return out.reshape(1, n_steps, d_model)

    return jax.shard_map(device_forward, mesh=mesh, in_specs=in_specs, out_specs=P('dp'), check_vma=False)
```

```python
import functools

import jax
import jax.numpy as jnp
from jax import lax
from jax.experimental import pallas as pl
from jax.experimental.pallas import tpu as pltpu
from jax.sharding import PartitionSpec as P

EPSILON = 1e-5
CHUNK = 128
PAIR = 128
HEAD_DIM = 64
HIGHEST = lax.Precision.HIGHEST
F32 = jnp.float32
BF16 = jnp.bfloat16

LAG_B, LAG_H, LAG_M, LAG_O, LAG_T, LAG_F1, LAG_F2 = 3, 3, 5, 7, 9, 11, 12
N_V, N_STAT, N_PAIR, N_HOP, N_TOT = 4, 8, 4, 8, 16
EARLY_TWO, EARLY_ONE = 2, 5
SUB = 1
SUB_ROWS = CHUNK // SUB
AHEAD = 4
VMEM_BYTES = 67043328
ROW_CONV, ROW_BIAS, ROW_NORM, ROW_GATE, ROW_SKIP, ROW_DT, ROW_A = 0, 4, 5, 6, 7, 8, 9


def fdot(a, b):
    return jnp.dot(a, b, precision=HIGHEST, preferred_element_type=F32)


def bdot(a, b):
    return jnp.dot(a, b, preferred_element_type=F32)


def kernel(n_chunks, n_layers, tp, inner_width,
           hid, wz, wx, wbc, wo, small_0, small_1, small_2, small_3, small_4, small_5, small_6, small_7, small_8, small_9, cur,
           wzv, wxv, wbcv, wdtv, dt_rows, wov, par, conv_in, state, vbuf, stat,
           obuf, pairbuf, hbuf, rbuf_a, rbuf_b, tbuf, halfbuf,
           norm_w, wdt, conv_x, conv_bc, bias_x, bias_bc, dt_bias, a_log, d_skip, gate_w,
           hid_sem, w_sem, small_sem,
           stat_send, stat_recv, pair_send, pair_recv, hop_send, hop_recv_a, hop_recv_b,
           tot_send_l, tot_send_r, tot_recv, half_send, half_recv):
    n_items = n_chunks * n_layers
    half = cur.shape[1] // 2
    width = wz.shape[-1]
    bc_width = wbc.shape[-1]
    heads = dt_bias.shape[-1]
    n_pairs = width // PAIR
    n_chips = tp // 2
    me = lax.axis_index('tp')
    z = me // 2
    core = me % 2
    partner = z * 2 + (1 - core)
    role = z + core * (n_chips - 1 - 2 * z)

    def on_line(k):
        return (k + core * (n_chips - 1 - 2 * k)) * 2 + core

    def remote(src, dst, send, recv, device):
        return pltpu.make_async_remote_copy(src_ref=src, dst_ref=dst, send_sem=send, recv_sem=recv, device_id={'tp': device}, device_id_type=pl.DeviceIdType.MESH)

    def chunk_rows(c):
        return pl.ds(pl.multiple_of(c * CHUNK, CHUNK), CHUNK)

    def hid_copy(c):
        return pltpu.make_async_copy(hid.at[chunk_rows(c), :], cur.at[chunk_rows(c), :], hid_sem.at[c])

    def w_copies(l):
        return [
            pltpu.make_async_copy(wz.at[l], wzv.at[l], w_sem.at[l, 0]),
            pltpu.make_async_copy(wx.at[l], wxv.at[l], w_sem.at[l, 1]),
            pltpu.make_async_copy(wbc.at[l], wbcv.at[l], w_sem.at[l, 2]),
            pltpu.make_async_copy(wo.at[l, :, pl.ds(0, half)], wov.at[l, 0], w_sem.at[l, 3]),
            pltpu.make_async_copy(wo.at[l, :, pl.ds(half, half)], wov.at[l, 1], w_sem.at[l, 4]),
        ]

    sources = (small_0, small_1, small_2, small_3, small_4, small_5, small_6, small_7, small_8, small_9)
    small = [pltpu.make_async_copy(src, dst, small_sem.at[k]) for k, (src, dst) in enumerate(zip(sources, (norm_w, wdt, conv_x, conv_bc, bias_x, bias_bc, dt_bias, a_log, d_skip, gate_w)))]
    for copy in small:
        copy.start()
    hid_copy(0).start()
    for copy in w_copies(0):
        copy.start()
    for c in range(1, AHEAD):
        hid_copy(c).start()

    barrier = pltpu.get_barrier_semaphore()
    for d in range(1, tp):
        pl.semaphore_signal(barrier, inc=1, device_id={'tp': (me + d) % tp}, device_id_type=pl.DeviceIdType.MESH)

    par[...] = jnp.zeros_like(par)
    dt_rows[...] = jnp.zeros_like(dt_rows)
    wdtv[...] = jnp.zeros_like(wdtv)
    for copy in small:
        copy.wait()
    for l in range(n_layers):
        par[l, ROW_CONV:ROW_CONV + 4, 0:width] = conv_x[l].astype(F32)
        par[l, ROW_CONV:ROW_CONV + 4, width:width + bc_width] = conv_bc[l].astype(F32)
        par[l, ROW_BIAS:ROW_BIAS + 1, 0:width] = bias_x[...].astype(F32)[l:l + 1]
        par[l, ROW_BIAS:ROW_BIAS + 1, width:width + bc_width] = bias_bc[...].astype(F32)[l:l + 1]
        par[l, ROW_NORM:ROW_NORM + 1, :] = norm_w[...].astype(F32)[l:l + 1]
        par[l, ROW_GATE:ROW_GATE + 1, 0:width] = gate_w[...].astype(F32)[l:l + 1]
        par[l, ROW_SKIP:ROW_SKIP + 1, 0:heads] = d_skip[l:l + 1, :]
        par[l, ROW_DT:ROW_DT + 1, 0:heads] = dt_bias[l:l + 1, :]
        par[l, ROW_A:ROW_A + 1, 0:heads] = a_log[l:l + 1, :]
        for n in range(heads):
            dt_rows[n:n + 1, :] = wdt[n].astype(F32)[l:l + 1]
        wdtv[l, 0:dt_rows.shape[0], :] = dt_rows[...].astype(BF16)
    pl.semaphore_wait(barrier, tp - 1)

    row_id = lax.broadcasted_iota(jnp.int32, (CHUNK, CHUNK), 0)
    col_id = lax.broadcasted_iota(jnp.int32, (CHUNK, CHUNK), 1)

    def stat_copy(m, d):
        slot = m % N_STAT
        return remote(stat.at[slot, me], stat.at[slot, me], stat_send.at[slot, d], stat_recv.at[slot, me], (me + d) % tp)

    def stat_arrival(m, d):
        slot = m % N_STAT
        peer = (me + d) % tp
        return remote(stat.at[slot, peer], stat.at[slot, peer], stat_send.at[slot, d], stat_recv.at[slot, peer], peer)

    def pair_copy(m):
        slot = m % N_PAIR
        return remote(obuf.at[slot], pairbuf.at[slot], pair_send.at[slot], pair_recv.at[slot], partner)

    def sub(s):
        return pl.ds(s * SUB_ROWS, SUB_ROWS)

    def hop_a(m, s, device):
        slot = m % N_HOP
        return remote(hbuf.at[slot, sub(s)], rbuf_a.at[slot, sub(s)], hop_send.at[slot, s], hop_recv_a.at[slot, s], device)

    def hop_b(m, s, device):
        slot = m % N_HOP
        return remote(hbuf.at[slot, sub(s)], rbuf_b.at[slot, sub(s)], hop_send.at[slot, s], hop_recv_b.at[slot, s], device)

    def tot_back(m, s, device):
        slot = m % N_TOT
        return remote(tbuf.at[slot, sub(s)], tbuf.at[slot, sub(s)], tot_send_l.at[slot, s], tot_recv.at[slot, s], device)

    def tot_on(m, s, device):
        slot = m % N_TOT
        return remote(tbuf.at[slot, sub(s)], tbuf.at[slot, sub(s)], tot_send_r.at[slot, s], tot_recv.at[slot, s], device)

    def half_copy(m, s):
        slot = m % N_PAIR
        return remote(tbuf.at[m % N_TOT, sub(s)], halfbuf.at[slot, sub(s)], half_send.at[slot, s], half_recv.at[slot, s], partner)

    def stage_a(m):
        l = m // n_chunks
        c = m % n_chunks

        @pl.when(l == 0)
        def _():
            hid_copy(c).wait()

        @pl.when(m + AHEAD < n_chunks)
        def _():
            hid_copy(m + AHEAD).start()

        for later in range(1, n_layers):
            @pl.when(m == later * AHEAD)
            def _(later=later):
                for copy in w_copies(later):
                    copy.start()

        @pl.when(c == 0)
        def _():
            for copy in w_copies(l):
                copy.wait()
            conv_in[0:8, :] = jnp.zeros((8, conv_in.shape[1]), F32)
            state[...] = jnp.zeros_like(state)

        rows = chunk_rows(c)
        u = cur[rows, :].astype(F32)
        scale = lax.rsqrt(jnp.mean(u * u, axis=-1, keepdims=True) + EPSILON)
        h = (u * scale * par[l, ROW_NORM:ROW_NORM + 1, :]).astype(BF16)
        gate_z = bdot(h, wzv[l]).astype(BF16).astype(F32)
        conv_in[8:8 + CHUNK, 0:width] = bdot(h, wxv[l]).astype(BF16).astype(F32)
        conv_in[8:8 + CHUNK, width:] = bdot(h, wbcv[l]).astype(BF16).astype(F32)
        dt_pre = lax.dot_general(h, wdtv[l], (((1,), (1,)), ((), ())), preferred_element_type=F32).astype(BF16).astype(F32)

        cw = conv_in.shape[1]
        conv = par[l, ROW_BIAS:ROW_BIAS + 1, 0:cw]
        for j in range(4):
            conv = conv + conv_in[5 + j:5 + j + CHUNK, :] * par[l, ROW_CONV + j:ROW_CONV + j + 1, 0:cw]
        act = conv * jax.nn.sigmoid(conv)
        conv_in[0:8, :] = conv_in[CHUNK:CHUNK + 8, :]
        n_state = (cw - width) // 2
        b_in = act[:, width:width + n_state]
        c_in = act[:, width + n_state:]

        pre = dt_pre + par[l, ROW_DT:ROW_DT + 1, 0:PAIR]
        dt = jnp.maximum(pre, 0.0) + jnp.log1p(jnp.exp(-jnp.abs(pre)))
        a = -dt * jnp.exp(par[l, ROW_A:ROW_A + 1, 0:PAIR])
        lower = row_id >= col_id
        a_cum = fdot(jnp.where(lower, 1.0, 0.0).astype(F32), a)
        a_cum_t = a_cum.T
        a_last = a_cum[CHUNK - 1:CHUNK, :]
        grow = jnp.exp(a_cum)
        tail = jnp.exp(a_last - a_cum)
        carry = jnp.exp(a_last)
        c_dot_b = lax.dot_general(c_in, b_in, (((1,), (1,)), ((), ())), precision=HIGHEST, preferred_element_type=F32)
        b_t = b_in.T
        first = lax.broadcasted_iota(jnp.int32, (1, PAIR), 1) < HEAD_DIM
        v_slot = m % N_V
        sq = jnp.zeros((CHUNK, PAIR), F32)
        skip = par[l, ROW_SKIP:ROW_SKIP + 1, 0:PAIR]
        for p in range(n_pairs):
            lanes = slice(p * PAIR, (p + 1) * PAIR)

            def spread(q):
                return jnp.where(first, q[:, 2 * p:2 * p + 1], q[:, 2 * p + 1:2 * p + 2])

            def mix(n):
                seg = a_cum[:, n:n + 1] - a_cum_t[n:n + 1, :]
                return jnp.where(lower, jnp.exp(jnp.minimum(seg, 0.0)), 0.0) * c_dot_b

            x = act[:, lanes]
            x_dt = x * spread(dt)
            y_in = jnp.where(first, fdot(mix(2 * p), x_dt), fdot(mix(2 * p + 1), x_dt))
            s_in = state[:, lanes]
            y_st = fdot(c_in, s_in) * spread(grow)
            state[:, lanes] = s_in * spread(carry) + fdot(b_t, x_dt * spread(tail))
            y = y_in + y_st + spread(skip) * x
            zp = gate_z[:, lanes]
            v = y * (zp * jax.nn.sigmoid(zp))
            vbuf[v_slot, :, lanes] = v
            sq = sq + v * v
        part = jnp.broadcast_to(jnp.sum(sq, axis=-1, keepdims=True), (CHUNK, PAIR)).T
        stat[m % N_STAT, me] = part[0:8, :]
        for d in range(1, tp):
            stat_copy(m, d).start()

    def stage_b(m):
        l = m // n_chunks
        for d in range(1, tp):
            stat_copy(m, d).wait_send()
            stat_arrival(m, d).wait_recv()
        slot = m % N_STAT
        total = stat[slot, 0]
        for s in range(1, tp):
            total = total + stat[slot, s]
        total = jnp.broadcast_to(total[0:1, :], (PAIR, CHUNK)).T
        scale = lax.rsqrt(total / inner_width + EPSILON)
        parts = []
        for p in range(n_pairs):
            lanes = slice(p * PAIR, (p + 1) * PAIR)
            parts.append((vbuf[m % N_V, :, lanes] * scale * par[l, ROW_GATE:ROW_GATE + 1, lanes]).astype(BF16))
        g = jnp.concatenate(parts, axis=1)
        obuf[m % N_PAIR] = bdot(g, wov[l, 1 - core])
        pair_copy(m).start()
        hbuf[m % N_HOP] = bdot(g, wov[l, core])

    def stage_h(m):
        pair_copy(m).wait()
        slot = m % N_HOP
        hbuf[slot] = hbuf[slot] + pairbuf[m % N_PAIR]

        @pl.when(role == 0)
        def _():
            for s in range(SUB):
                hop_a(m, s, on_line(1)).start()

        @pl.when(role == 3)
        def _():
            for s in range(SUB):
                hop_a(m, s, on_line(2)).start()

    def stage_m(m):
        @pl.when(role == 2)
        def _():
            slot = m % N_HOP
            for s in range(SUB):
                hop_a(m, s, on_line(3)).wait_recv()
                hbuf[slot, sub(s)] = hbuf[slot, sub(s)] + rbuf_a[slot, sub(s)]
                hop_b(m, s, on_line(1)).start()

    def stage_o(m):
        @pl.when(role == 1)
        def _():
            slot = m % N_HOP
            for s in range(SUB):
                hop_a(m, s, on_line(0)).wait_recv()
                hop_b(m, s, on_line(2)).wait_recv()
                tbuf[m % N_TOT, sub(s)] = rbuf_a[slot, sub(s)] + hbuf[slot, sub(s)] + rbuf_b[slot, sub(s)]
                tot_on(m, s, on_line(2)).start()
                tot_back(m, s, on_line(0)).start()

    def stage_t(m):
        @pl.when(role == 0)
        def _():
            for s in range(SUB):
                hop_a(m, s, on_line(1)).wait_send()
                tot_back(m, s, on_line(1)).wait_recv()

        @pl.when(role == 1)
        def _():
            for s in range(SUB):
                tot_back(m, s, on_line(0)).wait_send()
                tot_on(m, s, on_line(2)).wait_send()

        @pl.when(role == 2)
        def _():
            for s in range(SUB):
                hop_b(m, s, on_line(1)).wait_send()
                tot_on(m, s, on_line(1)).wait_recv()
                tot_on(m, s, on_line(3)).start()

        @pl.when(role == 3)
        def _():
            for s in range(SUB):
                hop_a(m, s, on_line(2)).wait_send()

    def stage_f1(m):
        for s in range(SUB):
            @pl.when(role == 3)
            def _(s=s):
                tot_on(m, s, on_line(2)).wait_recv()

            half_copy(m, s).start()

    def stage_f2(m):
        @pl.when(role == 2)
        def _():
            for s in range(SUB):
                tot_on(m, s, on_line(3)).wait_send()

        own = pl.ds(pl.multiple_of(core * half, PAIR), half)
        other = pl.ds(pl.multiple_of((1 - core) * half, PAIR), half)
        for s in range(SUB):
            half_copy(m, s).wait()
            rows = pl.ds(pl.multiple_of((m % n_chunks) * CHUNK + s * SUB_ROWS, SUB_ROWS), SUB_ROWS)
            cur[rows, own] = (cur[rows, own].astype(F32) + tbuf[m % N_TOT, sub(s)]).astype(BF16)
            cur[rows, other] = (cur[rows, other].astype(F32) + halfbuf[m % N_PAIR, sub(s)]).astype(BF16)

    def later_stage(i, lag, stage):
        k = i - lag
        item = jnp.where(k >= EARLY_ONE, k, jnp.where(k >= EARLY_TWO - 1, k + 1, k + 2))
        steady = jnp.logical_and(k >= EARLY_ONE, k < n_items)
        one_early = jnp.logical_and(k + 1 >= EARLY_TWO, k + 1 < EARLY_ONE)
        two_early = jnp.logical_and(k + 2 >= 0, k + 2 < EARLY_TWO)

        @pl.when(jnp.logical_or(steady, jnp.logical_or(one_early, two_early)))
        def _():
            stage(item)

    def step(i, carry):
        for lag, stage in ((LAG_F2, stage_f2), (LAG_F1, stage_f1), (LAG_T, stage_t), (LAG_O, stage_o), (LAG_M, stage_m), (LAG_B, stage_b)):
            later_stage(i, lag, stage)

        @pl.when(i < n_items)
        def _():
            stage_a(i)

        later_stage(i, LAG_H, stage_h)
        return carry

    lax.fori_loop(0, n_items + LAG_F2, step, 0)


def write_out(cur, out, sem):
    n_parts = sem.shape[0]
    rows = cur.shape[0] // n_parts
    copies = [pltpu.make_async_copy(cur.at[pl.ds(k * rows, rows)], out.at[pl.ds(k * rows, rows)], sem.at[k]) for k in range(n_parts)]
    for copy in copies:
        copy.start()
    for copy in copies:
        copy.wait()


def solution(mesh):
    tp = mesh.shape['tp']
    rep_spec = P()
    col_spec = P(None, None, 'tp')
    vec_spec = P(None, 'tp')
    in_specs = (P('dp'), rep_spec, col_spec, col_spec, rep_spec, col_spec, col_spec, rep_spec, vec_spec, rep_spec, vec_spec, vec_spec, vec_spec, vec_spec, P(None, 'tp', None))

    def device_forward(hidden, norm_w, w_z, w_x, w_bc, w_dt, conv_x, conv_bc, bias_x, bias_bc, dt_bias, a_log, d_skip, gate_w, w_out):
        n_layers, d_model, width = w_z.shape
        n_steps = hidden.shape[1]
        n_chunks = n_steps // CHUNK
        bc_width = w_bc.shape[-1]
        half = d_model // 2
        small = (norm_w, jnp.transpose(w_dt, (2, 0, 1)), conv_x, conv_bc, bias_x, bias_bc, dt_bias, a_log, d_skip, gate_w)
        hbm_spec = pl.BlockSpec(memory_space=pltpu.HBM)
        vmem_spec = pl.BlockSpec(memory_space=pltpu.VMEM)
        dma = pltpu.SemaphoreType.DMA
        block = (CHUNK, half)
        out = pl.pallas_call(
            functools.partial(kernel, n_chunks, n_layers, tp, width * tp),
            out_shape=pltpu.VMEM((n_steps, d_model), BF16),
            in_specs=[hbm_spec] * (5 + len(small)),
            out_specs=vmem_spec,
            scratch_shapes=[
                pltpu.VMEM((n_layers, d_model, width), BF16),
                pltpu.VMEM((n_layers, d_model, width), BF16),
                pltpu.VMEM((n_layers, d_model, bc_width), BF16),
                pltpu.VMEM((n_layers, PAIR, d_model), BF16),
                pltpu.VMEM((16, d_model), F32),
                pltpu.VMEM((n_layers, 2, width, half), BF16),
                pltpu.VMEM((n_layers, 16, d_model), F32),
                pltpu.VMEM((CHUNK + 8, width + bc_width), F32),
                pltpu.VMEM((bc_width // 2, width), F32),
                pltpu.VMEM((N_V, CHUNK, width), F32),
                pltpu.VMEM((N_STAT, tp, 8, CHUNK), F32),
                pltpu.VMEM((N_PAIR,) + block, F32),
                pltpu.VMEM((N_PAIR,) + block, F32),
                pltpu.VMEM((N_HOP,) + block, F32),
                pltpu.VMEM((N_HOP,) + block, F32),
                pltpu.VMEM((N_HOP,) + block, F32),
                pltpu.VMEM((N_TOT,) + block, F32),
                pltpu.VMEM((N_PAIR,) + block, F32),
                *[pltpu.VMEM(v.shape, v.dtype) for v in small],
                dma((n_chunks,)), dma((n_layers, 5)), dma((len(small),)),
                dma((N_STAT, tp)), dma((N_STAT, tp)), dma((N_PAIR,)), dma((N_PAIR,)),
                dma((N_HOP, SUB)), dma((N_HOP, SUB)), dma((N_HOP, SUB)),
                dma((N_TOT, SUB)), dma((N_TOT, SUB)), dma((N_TOT, SUB)), dma((N_PAIR, SUB)), dma((N_PAIR, SUB)),
            ],
            compiler_params=pltpu.CompilerParams(collective_id=0, has_side_effects=True, vmem_limit_bytes=VMEM_BYTES - 2 * n_steps * d_model),
        )(hidden.reshape(n_steps, d_model), w_z, w_x, w_bc, w_out, *small)
        out = pl.pallas_call(
            write_out,
            out_shape=jax.ShapeDtypeStruct((n_steps, d_model), BF16),
            in_specs=[vmem_spec],
            out_specs=hbm_spec,
            scratch_shapes=[dma((8,))],
            compiler_params=pltpu.CompilerParams(vmem_limit_bytes=1024 * 1024),
        )(out)
        return out.reshape(1, n_steps, d_model)

    return jax.shard_map(device_forward, mesh=mesh, in_specs=in_specs, out_specs=P('dp'), check_vma=False)
```

```python
import functools

import jax
import jax.numpy as jnp
from jax import lax
from jax.experimental import pallas as pl
from jax.experimental.pallas import tpu as pltpu
from jax.sharding import PartitionSpec as P

EPSILON = 1e-5
CHUNK = 128
PAIR = 128
HEAD_DIM = 64
HIGHEST = lax.Precision.HIGHEST
F32 = jnp.float32
BF16 = jnp.bfloat16

LAG_B, LAG_H, LAG_M, LAG_O, LAG_T, LAG_F1, LAG_F2 = 3, 4, 6, 8, 10, 12, 13
N_V, N_STAT, N_PAIR, N_HOP, N_TOT = 4, 8, 4, 8, 16
EARLY_TWO, EARLY_ONE = 2, 5
SUB = 4
SUB_ROWS = CHUNK // SUB
AHEAD = 4
VMEM_BYTES = 67043328
ROW_CONV, ROW_BIAS, ROW_NORM, ROW_GATE, ROW_SKIP, ROW_DT, ROW_A = 0, 4, 5, 6, 7, 8, 9


def fdot(a, b):
    return jnp.dot(a, b, precision=HIGHEST, preferred_element_type=F32)


def bdot(a, b):
    return jnp.dot(a, b, preferred_element_type=F32)


def kernel(n_chunks, n_layers, tp, inner_width,
           hid, wz, wx, wbc, wo, small_0, small_1, small_2, small_3, small_4, small_5, small_6, small_7, small_8, small_9, cur,
           wzv, wxv, wbcv, wdtv, dt_rows, wov, par, conv_in, state, vbuf, stat,
           obuf, pairbuf, hbuf, rbuf_a, rbuf_b, tbuf, halfbuf,
           norm_w, wdt, conv_x, conv_bc, bias_x, bias_bc, dt_bias, a_log, d_skip, gate_w,
           hid_sem, w_sem, small_sem,
           stat_send, stat_recv, pair_send, pair_recv, hop_send, hop_recv_a, hop_recv_b,
           tot_send_l, tot_send_r, tot_recv, half_send, half_recv):
    n_items = n_chunks * n_layers
    half = cur.shape[1] // 2
    width = wz.shape[-1]
    bc_width = wbc.shape[-1]
    heads = dt_bias.shape[-1]
    n_pairs = width // PAIR
    n_chips = tp // 2
    me = lax.axis_index('tp')
    z = me // 2
    core = me % 2
    partner = z * 2 + (1 - core)
    role = z + core * (n_chips - 1 - 2 * z)

    def on_line(k):
        return (k + core * (n_chips - 1 - 2 * k)) * 2 + core

    def remote(src, dst, send, recv, device):
        return pltpu.make_async_remote_copy(src_ref=src, dst_ref=dst, send_sem=send, recv_sem=recv, device_id={'tp': device}, device_id_type=pl.DeviceIdType.MESH)

    def chunk_rows(c):
        return pl.ds(pl.multiple_of(c * CHUNK, CHUNK), CHUNK)

    def hid_copy(c):
        return pltpu.make_async_copy(hid.at[chunk_rows(c), :], cur.at[chunk_rows(c), :], hid_sem.at[c])

    def w_copies(l):
        return [
            pltpu.make_async_copy(wz.at[l], wzv.at[l], w_sem.at[l, 0]),
            pltpu.make_async_copy(wx.at[l], wxv.at[l], w_sem.at[l, 1]),
            pltpu.make_async_copy(wbc.at[l], wbcv.at[l], w_sem.at[l, 2]),
            pltpu.make_async_copy(wo.at[l, :, pl.ds(0, half)], wov.at[l, 0], w_sem.at[l, 3]),
            pltpu.make_async_copy(wo.at[l, :, pl.ds(half, half)], wov.at[l, 1], w_sem.at[l, 4]),
        ]

    sources = (small_0, small_1, small_2, small_3, small_4, small_5, small_6, small_7, small_8, small_9)
    small = [pltpu.make_async_copy(src, dst, small_sem.at[k]) for k, (src, dst) in enumerate(zip(sources, (norm_w, wdt, conv_x, conv_bc, bias_x, bias_bc, dt_bias, a_log, d_skip, gate_w)))]
    for copy in small:
        copy.start()
    hid_copy(0).start()
    for copy in w_copies(0):
        copy.start()
    for c in range(1, AHEAD):
        hid_copy(c).start()

    barrier = pltpu.get_barrier_semaphore()
    for d in range(1, tp):
        pl.semaphore_signal(barrier, inc=1, device_id={'tp': (me + d) % tp}, device_id_type=pl.DeviceIdType.MESH)

    par[...] = jnp.zeros_like(par)
    dt_rows[...] = jnp.zeros_like(dt_rows)
    wdtv[...] = jnp.zeros_like(wdtv)
    for copy in small:
        copy.wait()
    for l in range(n_layers):
        par[l, ROW_CONV:ROW_CONV + 4, 0:width] = conv_x[l].astype(F32)
        par[l, ROW_CONV:ROW_CONV + 4, width:width + bc_width] = conv_bc[l].astype(F32)
        par[l, ROW_BIAS:ROW_BIAS + 1, 0:width] = bias_x[...].astype(F32)[l:l + 1]
        par[l, ROW_BIAS:ROW_BIAS + 1, width:width + bc_width] = bias_bc[...].astype(F32)[l:l + 1]
        par[l, ROW_NORM:ROW_NORM + 1, :] = norm_w[...].astype(F32)[l:l + 1]
        par[l, ROW_GATE:ROW_GATE + 1, 0:width] = gate_w[...].astype(F32)[l:l + 1]
        par[l, ROW_SKIP:ROW_SKIP + 1, 0:heads] = d_skip[l:l + 1, :]
        par[l, ROW_DT:ROW_DT + 1, 0:heads] = dt_bias[l:l + 1, :]
        par[l, ROW_A:ROW_A + 1, 0:heads] = a_log[l:l + 1, :]
        for n in range(heads):
            dt_rows[n:n + 1, :] = wdt[n].astype(F32)[l:l + 1]
        wdtv[l, 0:dt_rows.shape[0], :] = dt_rows[...].astype(BF16)
    pl.semaphore_wait(barrier, tp - 1)

    row_id = lax.broadcasted_iota(jnp.int32, (CHUNK, CHUNK), 0)
    col_id = lax.broadcasted_iota(jnp.int32, (CHUNK, CHUNK), 1)

    def stat_copy(m, d):
        slot = m % N_STAT
        return remote(stat.at[slot, me], stat.at[slot, me], stat_send.at[slot, d], stat_recv.at[slot, me], (me + d) % tp)

    def stat_arrival(m, d):
        slot = m % N_STAT
        peer = (me + d) % tp
        return remote(stat.at[slot, peer], stat.at[slot, peer], stat_send.at[slot, d], stat_recv.at[slot, peer], peer)

    def pair_copy(m):
        slot = m % N_PAIR
        return remote(obuf.at[slot], pairbuf.at[slot], pair_send.at[slot], pair_recv.at[slot], partner)

    def sub(s):
        return pl.ds(s * SUB_ROWS, SUB_ROWS)

    def hop_a(m, s, device):
        slot = m % N_HOP
        return remote(hbuf.at[slot, sub(s)], rbuf_a.at[slot, sub(s)], hop_send.at[slot, s], hop_recv_a.at[slot, s], device)

    def hop_b(m, s, device):
        slot = m % N_HOP
        return remote(hbuf.at[slot, sub(s)], rbuf_b.at[slot, sub(s)], hop_send.at[slot, s], hop_recv_b.at[slot, s], device)

    def tot_back(m, s, device):
        slot = m % N_TOT
        return remote(tbuf.at[slot, sub(s)], tbuf.at[slot, sub(s)], tot_send_l.at[slot, s], tot_recv.at[slot, s], device)

    def tot_on(m, s, device):
        slot = m % N_TOT
        return remote(tbuf.at[slot, sub(s)], tbuf.at[slot, sub(s)], tot_send_r.at[slot, s], tot_recv.at[slot, s], device)

    def half_copy(m, s):
        slot = m % N_PAIR
        return remote(tbuf.at[m % N_TOT, sub(s)], halfbuf.at[slot, sub(s)], half_send.at[slot, s], half_recv.at[slot, s], partner)

    def stage_a(m):
        l = m // n_chunks
        c = m % n_chunks

        @pl.when(l == 0)
        def _():
            hid_copy(c).wait()

        @pl.when(m + AHEAD < n_chunks)
        def _():
            hid_copy(m + AHEAD).start()

        for later in range(1, n_layers):
            @pl.when(m == later * AHEAD)
            def _(later=later):
                for copy in w_copies(later):
                    copy.start()

        @pl.when(c == 0)
        def _():
            for copy in w_copies(l):
                copy.wait()
            conv_in[0:8, :] = jnp.zeros((8, conv_in.shape[1]), F32)
            state[...] = jnp.zeros_like(state)

        rows = chunk_rows(c)
        u = cur[rows, :].astype(F32)
        scale = lax.rsqrt(jnp.mean(u * u, axis=-1, keepdims=True) + EPSILON)
        h = (u * scale * par[l, ROW_NORM:ROW_NORM + 1, :]).astype(BF16)
        gate_z = bdot(h, wzv[l]).astype(BF16).astype(F32)
        conv_in[8:8 + CHUNK, 0:width] = bdot(h, wxv[l]).astype(BF16).astype(F32)
        conv_in[8:8 + CHUNK, width:] = bdot(h, wbcv[l]).astype(BF16).astype(F32)
        dt_pre = lax.dot_general(h, wdtv[l], (((1,), (1,)), ((), ())), preferred_element_type=F32).astype(BF16).astype(F32)

        cw = conv_in.shape[1]
        conv = par[l, ROW_BIAS:ROW_BIAS + 1, 0:cw]
        for j in range(4):
            conv = conv + conv_in[5 + j:5 + j + CHUNK, :] * par[l, ROW_CONV + j:ROW_CONV + j + 1, 0:cw]
        act = conv * jax.nn.sigmoid(conv)
        conv_in[0:8, :] = conv_in[CHUNK:CHUNK + 8, :]
        n_state = (cw - width) // 2
        b_in = act[:, width:width + n_state]
        c_in = act[:, width + n_state:]

        pre = dt_pre + par[l, ROW_DT:ROW_DT + 1, 0:PAIR]
        dt = jnp.maximum(pre, 0.0) + jnp.log1p(jnp.exp(-jnp.abs(pre)))
        a = -dt * jnp.exp(par[l, ROW_A:ROW_A + 1, 0:PAIR])
        lower = row_id >= col_id
        a_cum = fdot(jnp.where(lower, 1.0, 0.0).astype(F32), a)
        a_cum_t = a_cum.T
        a_last = a_cum[CHUNK - 1:CHUNK, :]
        grow = jnp.exp(a_cum)
        tail = jnp.exp(a_last - a_cum)
        carry = jnp.exp(a_last)
        c_dot_b = lax.dot_general(c_in, b_in, (((1,), (1,)), ((), ())), precision=HIGHEST, preferred_element_type=F32)
        b_t = b_in.T
        first = lax.broadcasted_iota(jnp.int32, (1, PAIR), 1) < HEAD_DIM
        v_slot = m % N_V
        sq = jnp.zeros((CHUNK, PAIR), F32)
        skip = par[l, ROW_SKIP:ROW_SKIP + 1, 0:PAIR]
        for p in range(n_pairs):
            lanes = slice(p * PAIR, (p + 1) * PAIR)

            def spread(q):
                return jnp.where(first, q[:, 2 * p:2 * p + 1], q[:, 2 * p + 1:2 * p + 2])

            def mix(n):
                seg = a_cum[:, n:n + 1] - a_cum_t[n:n + 1, :]
                return jnp.where(lower, jnp.exp(jnp.minimum(seg, 0.0)), 0.0) * c_dot_b

            x = act[:, lanes]
            x_dt = x * spread(dt)
            y_in = jnp.where(first, fdot(mix(2 * p), x_dt), fdot(mix(2 * p + 1), x_dt))
            s_in = state[:, lanes]
            y_st = fdot(c_in, s_in) * spread(grow)
            state[:, lanes] = s_in * spread(carry) + fdot(b_t, x_dt * spread(tail))
            y = y_in + y_st + spread(skip) * x
            zp = gate_z[:, lanes]
            v = y * (zp * jax.nn.sigmoid(zp))
            vbuf[v_slot, :, lanes] = v
            sq = sq + v * v
        part = jnp.broadcast_to(jnp.sum(sq, axis=-1, keepdims=True), (CHUNK, PAIR)).T
        stat[m % N_STAT, me] = part[0:1, :]
        for d in range(1, tp):
            stat_copy(m, d).start()

    def stage_b(m):
        l = m // n_chunks
        for d in range(1, tp):
            stat_copy(m, d).wait_send()
            stat_arrival(m, d).wait_recv()
        slot = m % N_STAT
        total = stat[slot, 0]
        for s in range(1, tp):
            total = total + stat[slot, s]
        total = jnp.broadcast_to(total, (PAIR, CHUNK)).T
        scale = lax.rsqrt(total / inner_width + EPSILON)
        parts = []
        for p in range(n_pairs):
            lanes = slice(p * PAIR, (p + 1) * PAIR)
            parts.append((vbuf[m % N_V, :, lanes] * scale * par[l, ROW_GATE:ROW_GATE + 1, lanes]).astype(BF16))
        g = jnp.concatenate(parts, axis=1)
        obuf[m % N_PAIR] = bdot(g, wov[l, 1 - core])
        pair_copy(m).start()
        hbuf[m % N_HOP] = bdot(g, wov[l, core])

    def stage_h(m):
        pair_copy(m).wait()
        slot = m % N_HOP
        hbuf[slot] = hbuf[slot] + pairbuf[m % N_PAIR]

        @pl.when(role == 0)
        def _():
            for s in range(SUB):
                hop_a(m, s, on_line(1)).start()

        @pl.when(role == 3)
        def _():
            for s in range(SUB):
                hop_a(m, s, on_line(2)).start()

    def stage_m(m):
        @pl.when(role == 2)
        def _():
            slot = m % N_HOP
            for s in range(SUB):
                hop_a(m, s, on_line(3)).wait_recv()
                hbuf[slot, sub(s)] = hbuf[slot, sub(s)] + rbuf_a[slot, sub(s)]
                hop_b(m, s, on_line(1)).start()

    def stage_o(m):
        @pl.when(role == 1)
        def _():
            slot = m % N_HOP
            for s in range(SUB):
                hop_a(m, s, on_line(0)).wait_recv()
                hop_b(m, s, on_line(2)).wait_recv()
                tbuf[m % N_TOT, sub(s)] = rbuf_a[slot, sub(s)] + hbuf[slot, sub(s)] + rbuf_b[slot, sub(s)]
                tot_on(m, s, on_line(2)).start()
                tot_back(m, s, on_line(0)).start()

    def stage_t(m):
        @pl.when(role == 0)
        def _():
            for s in range(SUB):
                hop_a(m, s, on_line(1)).wait_send()
                tot_back(m, s, on_line(1)).wait_recv()

        @pl.when(role == 1)
        def _():
            for s in range(SUB):
                tot_back(m, s, on_line(0)).wait_send()
                tot_on(m, s, on_line(2)).wait_send()

        @pl.when(role == 2)
        def _():
            for s in range(SUB):
                hop_b(m, s, on_line(1)).wait_send()
                tot_on(m, s, on_line(1)).wait_recv()
                tot_on(m, s, on_line(3)).start()

        @pl.when(role == 3)
        def _():
            for s in range(SUB):
                hop_a(m, s, on_line(2)).wait_send()

    def stage_f1(m):
        for s in range(SUB):
            @pl.when(role == 3)
            def _(s=s):
                tot_on(m, s, on_line(2)).wait_recv()

            half_copy(m, s).start()

    def stage_f2(m):
        @pl.when(role == 2)
        def _():
            for s in range(SUB):
                tot_on(m, s, on_line(3)).wait_send()

        own = pl.ds(pl.multiple_of(core * half, PAIR), half)
        other = pl.ds(pl.multiple_of((1 - core) * half, PAIR), half)
        for s in range(SUB):
            half_copy(m, s).wait()
            rows = pl.ds(pl.multiple_of((m % n_chunks) * CHUNK + s * SUB_ROWS, SUB_ROWS), SUB_ROWS)
            cur[rows, own] = (cur[rows, own].astype(F32) + tbuf[m % N_TOT, sub(s)]).astype(BF16)
            cur[rows, other] = (cur[rows, other].astype(F32) + halfbuf[m % N_PAIR, sub(s)]).astype(BF16)

    def step(i, carry):
        for lag, stage in ((LAG_F2, stage_f2), (LAG_F1, stage_f1), (LAG_T, stage_t), (LAG_O, stage_o), (LAG_M, stage_m), (LAG_H, stage_h), (LAG_B, stage_b)):
            k = i - lag
            item = jnp.where(k >= EARLY_ONE, k, jnp.where(k >= EARLY_TWO - 1, k + 1, k + 2))
            steady = jnp.logical_and(k >= EARLY_ONE, k < n_items)
            one_early = jnp.logical_and(k + 1 >= EARLY_TWO, k + 1 < EARLY_ONE)
            two_early = jnp.logical_and(k + 2 >= 0, k + 2 < EARLY_TWO)

            @pl.when(jnp.logical_or(steady, jnp.logical_or(one_early, two_early)))
            def _(item=item, stage=stage):
                stage(item)

        @pl.when(i < n_items)
        def _():
            stage_a(i)
        return carry

    lax.fori_loop(0, n_items + LAG_F2, step, 0)


def write_out(cur, out, sem):
    n_parts = sem.shape[0]
    rows = cur.shape[0] // n_parts
    copies = [pltpu.make_async_copy(cur.at[pl.ds(k * rows, rows)], out.at[pl.ds(k * rows, rows)], sem.at[k]) for k in range(n_parts)]
    for copy in copies:
        copy.start()
    for copy in copies:
        copy.wait()


def solution(mesh):
    tp = mesh.shape['tp']
    rep_spec = P()
    col_spec = P(None, None, 'tp')
    vec_spec = P(None, 'tp')
    in_specs = (P('dp'), rep_spec, col_spec, col_spec, rep_spec, col_spec, col_spec, rep_spec, vec_spec, rep_spec, vec_spec, vec_spec, vec_spec, vec_spec, P(None, 'tp', None))

    def device_forward(hidden, norm_w, w_z, w_x, w_bc, w_dt, conv_x, conv_bc, bias_x, bias_bc, dt_bias, a_log, d_skip, gate_w, w_out):
        n_layers, d_model, width = w_z.shape
        n_steps = hidden.shape[1]
        n_chunks = n_steps // CHUNK
        bc_width = w_bc.shape[-1]
        half = d_model // 2
        small = (norm_w, jnp.transpose(w_dt, (2, 0, 1)), conv_x, conv_bc, bias_x, bias_bc, dt_bias, a_log, d_skip, gate_w)
        hbm_spec = pl.BlockSpec(memory_space=pltpu.HBM)
        vmem_spec = pl.BlockSpec(memory_space=pltpu.VMEM)
        dma = pltpu.SemaphoreType.DMA
        block = (CHUNK, half)
        out = pl.pallas_call(
            functools.partial(kernel, n_chunks, n_layers, tp, width * tp),
            out_shape=pltpu.VMEM((n_steps, d_model), BF16),
            in_specs=[hbm_spec] * (5 + len(small)),
            out_specs=vmem_spec,
            scratch_shapes=[
                pltpu.VMEM((n_layers, d_model, width), BF16),
                pltpu.VMEM((n_layers, d_model, width), BF16),
                pltpu.VMEM((n_layers, d_model, bc_width), BF16),
                pltpu.VMEM((n_layers, PAIR, d_model), BF16),
                pltpu.VMEM((16, d_model), F32),
                pltpu.VMEM((n_layers, 2, width, half), BF16),
                pltpu.VMEM((n_layers, 16, d_model), F32),
                pltpu.VMEM((CHUNK + 8, width + bc_width), F32),
                pltpu.VMEM((bc_width // 2, width), F32),
                pltpu.VMEM((N_V, CHUNK, width), F32),
                pltpu.VMEM((N_STAT, tp, 1, CHUNK), F32),
                pltpu.VMEM((N_PAIR,) + block, F32),
                pltpu.VMEM((N_PAIR,) + block, F32),
                pltpu.VMEM((N_HOP,) + block, F32),
                pltpu.VMEM((N_HOP,) + block, F32),
                pltpu.VMEM((N_HOP,) + block, F32),
                pltpu.VMEM((N_TOT,) + block, F32),
                pltpu.VMEM((N_PAIR,) + block, F32),
                *[pltpu.VMEM(v.shape, v.dtype) for v in small],
                dma((n_chunks,)), dma((n_layers, 5)), dma((len(small),)),
                dma((N_STAT, tp)), dma((N_STAT, tp)), dma((N_PAIR,)), dma((N_PAIR,)),
                dma((N_HOP, SUB)), dma((N_HOP, SUB)), dma((N_HOP, SUB)),
                dma((N_TOT, SUB)), dma((N_TOT, SUB)), dma((N_TOT, SUB)), dma((N_PAIR, SUB)), dma((N_PAIR, SUB)),
            ],
            compiler_params=pltpu.CompilerParams(collective_id=0, has_side_effects=True, vmem_limit_bytes=VMEM_BYTES - 2 * n_steps * d_model),
        )(hidden.reshape(n_steps, d_model), w_z, w_x, w_bc, w_out, *small)
        out = pl.pallas_call(
            write_out,
            out_shape=jax.ShapeDtypeStruct((n_steps, d_model), BF16),
            in_specs=[vmem_spec],
            out_specs=hbm_spec,
            scratch_shapes=[dma((8,))],
            compiler_params=pltpu.CompilerParams(vmem_limit_bytes=1024 * 1024),
        )(out)
        return out.reshape(1, n_steps, d_model)

    return jax.shard_map(device_forward, mesh=mesh, in_specs=in_specs, out_specs=P('dp'), check_vma=False)
```

```python
import functools

import jax
import jax.numpy as jnp
from jax import lax
from jax.experimental import pallas as pl
from jax.experimental.pallas import tpu as pltpu
from jax.sharding import PartitionSpec as P

EPSILON = 1e-5
CHUNK = 128
PAIR = 128
HEAD_DIM = 64
HIGHEST = lax.Precision.HIGHEST
F32 = jnp.float32
BF16 = jnp.bfloat16

LAG_B, LAG_H, LAG_M, LAG_O, LAG_T, LAG_F1, LAG_F2 = 3, 4, 6, 7, 8, 9, 10
N_V, N_STAT, N_PAIR, N_HOP, N_TOT = 4, 8, 4, 8, 16
EARLY_TWO, EARLY_ONE = 2, 5
SUB = 4
SUB_ROWS = CHUNK // SUB
AHEAD = 4
VMEM_BYTES = 67043328
ROW_CONV, ROW_BIAS, ROW_NORM, ROW_GATE, ROW_SKIP, ROW_DT, ROW_A = 0, 4, 5, 6, 7, 8, 9


def fdot(a, b):
    return jnp.dot(a, b, precision=HIGHEST, preferred_element_type=F32)


def bdot(a, b):
    return jnp.dot(a, b, preferred_element_type=F32)


def kernel(n_chunks, n_layers, tp, inner_width,
           hid, wz, wx, wbc, wo, small_0, small_1, small_2, small_3, small_4, small_5, small_6, small_7, small_8, small_9, cur,
           wzv, wxv, wbcv, wdtv, dt_rows, wov, par, conv_in, state, vbuf, stat,
           obuf, pairbuf, hbuf, rbuf_a, rbuf_b, tbuf, halfbuf,
           norm_w, wdt, conv_x, conv_bc, bias_x, bias_bc, dt_bias, a_log, d_skip, gate_w,
           hid_sem, w_sem, small_sem,
           stat_send, stat_recv, pair_send, pair_recv, hop_send, hop_recv_a, hop_recv_b,
           tot_send_l, tot_send_r, tot_recv, half_send, half_recv):
    n_items = n_chunks * n_layers
    half = cur.shape[1] // 2
    width = wz.shape[-1]
    bc_width = wbc.shape[-1]
    heads = dt_bias.shape[-1]
    n_pairs = width // PAIR
    n_chips = tp // 2
    me = lax.axis_index('tp')
    z = me // 2
    core = me % 2
    partner = z * 2 + (1 - core)
    role = z + core * (n_chips - 1 - 2 * z)

    def on_line(k):
        return (k + core * (n_chips - 1 - 2 * k)) * 2 + core

    def remote(src, dst, send, recv, device):
        return pltpu.make_async_remote_copy(src_ref=src, dst_ref=dst, send_sem=send, recv_sem=recv, device_id={'tp': device}, device_id_type=pl.DeviceIdType.MESH)

    def chunk_rows(c):
        return pl.ds(pl.multiple_of(c * CHUNK, CHUNK), CHUNK)

    def hid_copy(c):
        return pltpu.make_async_copy(hid.at[chunk_rows(c), :], cur.at[chunk_rows(c), :], hid_sem.at[c])

    def w_copies(l):
        return [
            pltpu.make_async_copy(wz.at[l], wzv.at[l], w_sem.at[l, 0]),
            pltpu.make_async_copy(wx.at[l], wxv.at[l], w_sem.at[l, 1]),
            pltpu.make_async_copy(wbc.at[l], wbcv.at[l], w_sem.at[l, 2]),
            pltpu.make_async_copy(wo.at[l, :, pl.ds(0, half)], wov.at[l, 0], w_sem.at[l, 3]),
            pltpu.make_async_copy(wo.at[l, :, pl.ds(half, half)], wov.at[l, 1], w_sem.at[l, 4]),
        ]

    sources = (small_0, small_1, small_2, small_3, small_4, small_5, small_6, small_7, small_8, small_9)
    small = [pltpu.make_async_copy(src, dst, small_sem.at[k]) for k, (src, dst) in enumerate(zip(sources, (norm_w, wdt, conv_x, conv_bc, bias_x, bias_bc, dt_bias, a_log, d_skip, gate_w)))]
    for copy in small:
        copy.start()
    hid_copy(0).start()
    for copy in w_copies(0):
        copy.start()
    for c in range(1, AHEAD):
        hid_copy(c).start()

    barrier = pltpu.get_barrier_semaphore()
    for d in range(1, tp):
        pl.semaphore_signal(barrier, inc=1, device_id={'tp': (me + d) % tp}, device_id_type=pl.DeviceIdType.MESH)

    par[...] = jnp.zeros_like(par)
    dt_rows[...] = jnp.zeros_like(dt_rows)
    wdtv[...] = jnp.zeros_like(wdtv)
    for copy in small:
        copy.wait()
    for l in range(n_layers):
        par[l, ROW_CONV:ROW_CONV + 4, 0:width] = conv_x[l].astype(F32)
        par[l, ROW_CONV:ROW_CONV + 4, width:width + bc_width] = conv_bc[l].astype(F32)
        par[l, ROW_BIAS:ROW_BIAS + 1, 0:width] = bias_x[...].astype(F32)[l:l + 1]
        par[l, ROW_BIAS:ROW_BIAS + 1, width:width + bc_width] = bias_bc[...].astype(F32)[l:l + 1]
        par[l, ROW_NORM:ROW_NORM + 1, :] = norm_w[...].astype(F32)[l:l + 1]
        par[l, ROW_GATE:ROW_GATE + 1, 0:width] = gate_w[...].astype(F32)[l:l + 1]
        par[l, ROW_SKIP:ROW_SKIP + 1, 0:heads] = d_skip[l:l + 1, :]
        par[l, ROW_DT:ROW_DT + 1, 0:heads] = dt_bias[l:l + 1, :]
        par[l, ROW_A:ROW_A + 1, 0:heads] = a_log[l:l + 1, :]
        for n in range(heads):
            dt_rows[n:n + 1, :] = wdt[n].astype(F32)[l:l + 1]
        wdtv[l, 0:dt_rows.shape[0], :] = dt_rows[...].astype(BF16)

    row_id = lax.broadcasted_iota(jnp.int32, (CHUNK, CHUNK), 0)
    col_id = lax.broadcasted_iota(jnp.int32, (CHUNK, CHUNK), 1)

    def stat_copy(m, d):
        slot = m % N_STAT
        return remote(stat.at[slot, me], stat.at[slot, me], stat_send.at[slot, d], stat_recv.at[slot, me], (me + d) % tp)

    def stat_arrival(m, d):
        slot = m % N_STAT
        peer = (me + d) % tp
        return remote(stat.at[slot, peer], stat.at[slot, peer], stat_send.at[slot, d], stat_recv.at[slot, peer], peer)

    def pair_copy(m):
        slot = m % N_PAIR
        return remote(obuf.at[slot], pairbuf.at[slot], pair_send.at[slot], pair_recv.at[slot], partner)

    def sub(s):
        return pl.ds(s * SUB_ROWS, SUB_ROWS)

    def hop_a(m, s, device):
        slot = m % N_HOP
        return remote(hbuf.at[slot, sub(s)], rbuf_a.at[slot, sub(s)], hop_send.at[slot, s], hop_recv_a.at[slot, s], device)

    def hop_b(m, s, device):
        slot = m % N_HOP
        return remote(hbuf.at[slot, sub(s)], rbuf_b.at[slot, sub(s)], hop_send.at[slot, s], hop_recv_b.at[slot, s], device)

    def tot_back(m, s, device):
        slot = m % N_TOT
        return remote(tbuf.at[slot, sub(s)], tbuf.at[slot, sub(s)], tot_send_l.at[slot, s], tot_recv.at[slot, s], device)

    def tot_on(m, s, device):
        slot = m % N_TOT
        return remote(tbuf.at[slot, sub(s)], tbuf.at[slot, sub(s)], tot_send_r.at[slot, s], tot_recv.at[slot, s], device)

    def half_copy(m, s):
        slot = m % N_PAIR
        return remote(tbuf.at[m % N_TOT, sub(s)], halfbuf.at[slot, sub(s)], half_send.at[slot, s], half_recv.at[slot, s], partner)

    def stage_a(m, before_send=None):
        l = m // n_chunks
        c = m % n_chunks

        @pl.when(l == 0)
        def _():
            hid_copy(c).wait()

        @pl.when(m + AHEAD < n_chunks)
        def _():
            hid_copy(m + AHEAD).start()

        for later in range(1, n_layers):
            @pl.when(m == later * AHEAD)
            def _(later=later):
                for copy in w_copies(later):
                    copy.start()

        @pl.when(c == 0)
        def _():
            for copy in w_copies(l):
                copy.wait()
            conv_in[0:8, :] = jnp.zeros((8, conv_in.shape[1]), F32)
            state[...] = jnp.zeros_like(state)

        rows = chunk_rows(c)
        u = cur[rows, :].astype(F32)
        scale = lax.rsqrt(jnp.mean(u * u, axis=-1, keepdims=True) + EPSILON)
        h = (u * scale * par[l, ROW_NORM:ROW_NORM + 1, :]).astype(BF16)
        gate_z = bdot(h, wzv[l]).astype(BF16).astype(F32)
        conv_in[8:8 + CHUNK, 0:width] = bdot(h, wxv[l]).astype(BF16).astype(F32)
        conv_in[8:8 + CHUNK, width:] = bdot(h, wbcv[l]).astype(BF16).astype(F32)
        dt_pre = lax.dot_general(h, wdtv[l], (((1,), (1,)), ((), ())), preferred_element_type=F32).astype(BF16).astype(F32)

        cw = conv_in.shape[1]
        conv = par[l, ROW_BIAS:ROW_BIAS + 1, 0:cw]
        for j in range(4):
            conv = conv + conv_in[5 + j:5 + j + CHUNK, :] * par[l, ROW_CONV + j:ROW_CONV + j + 1, 0:cw]
        act = conv * jax.nn.sigmoid(conv)
        conv_in[0:8, :] = conv_in[CHUNK:CHUNK + 8, :]
        n_state = (cw - width) // 2
        b_in = act[:, width:width + n_state]
        c_in = act[:, width + n_state:]

        pre = dt_pre + par[l, ROW_DT:ROW_DT + 1, 0:PAIR]
        dt = jnp.maximum(pre, 0.0) + jnp.log1p(jnp.exp(-jnp.abs(pre)))
        a = -dt * jnp.exp(par[l, ROW_A:ROW_A + 1, 0:PAIR])
        lower = row_id >= col_id
        a_cum = fdot(jnp.where(lower, 1.0, 0.0).astype(F32), a)
        a_cum_t = a_cum.T
        a_last = a_cum[CHUNK - 1:CHUNK, :]
        grow = jnp.exp(a_cum)
        tail = jnp.exp(a_last - a_cum)
        carry = jnp.exp(a_last)
        c_dot_b = lax.dot_general(c_in, b_in, (((1,), (1,)), ((), ())), precision=HIGHEST, preferred_element_type=F32)
        b_t = b_in.T
        first = lax.broadcasted_iota(jnp.int32, (1, PAIR), 1) < HEAD_DIM
        v_slot = m % N_V
        sq = jnp.zeros((CHUNK, PAIR), F32)
        skip = par[l, ROW_SKIP:ROW_SKIP + 1, 0:PAIR]
        for p in range(n_pairs):
            lanes = slice(p * PAIR, (p + 1) * PAIR)

            def spread(q):
                return jnp.where(first, q[:, 2 * p:2 * p + 1], q[:, 2 * p + 1:2 * p + 2])

            def mix(n):
                seg = a_cum[:, n:n + 1] - a_cum_t[n:n + 1, :]
                return jnp.where(lower, jnp.exp(jnp.minimum(seg, 0.0)), 0.0) * c_dot_b

            x = act[:, lanes]
            x_dt = x * spread(dt)
            y_in = jnp.where(first, fdot(mix(2 * p), x_dt), fdot(mix(2 * p + 1), x_dt))
            s_in = state[:, lanes]
            y_st = fdot(c_in, s_in) * spread(grow)
            state[:, lanes] = s_in * spread(carry) + fdot(b_t, x_dt * spread(tail))
            y = y_in + y_st + spread(skip) * x
            zp = gate_z[:, lanes]
            v = y * (zp * jax.nn.sigmoid(zp))
            vbuf[v_slot, :, lanes] = v
            sq = sq + v * v
        part = jnp.broadcast_to(jnp.sum(sq, axis=-1, keepdims=True), (CHUNK, PAIR)).T
        stat[m % N_STAT, me] = part[0:1, :]
        if before_send is not None:
            before_send()
        for d in range(1, tp):
            stat_copy(m, d).start()

    def stage_b(m):
        l = m // n_chunks
        for d in range(1, tp):
            stat_copy(m, d).wait_send()
            stat_arrival(m, d).wait_recv()
        slot = m % N_STAT
        total = stat[slot, 0]
        for s in range(1, tp):
            total = total + stat[slot, s]
        total = jnp.broadcast_to(total, (PAIR, CHUNK)).T
        scale = lax.rsqrt(total / inner_width + EPSILON)
        parts = []
        for p in range(n_pairs):
            lanes = slice(p * PAIR, (p + 1) * PAIR)
            parts.append((vbuf[m % N_V, :, lanes] * scale * par[l, ROW_GATE:ROW_GATE + 1, lanes]).astype(BF16))
        g = jnp.concatenate(parts, axis=1)
        obuf[m % N_PAIR] = bdot(g, wov[l, 1 - core])
        pair_copy(m).start()
        hbuf[m % N_HOP] = bdot(g, wov[l, core])

    def stage_h(m):
        pair_copy(m).wait()
        slot = m % N_HOP
        hbuf[slot] = hbuf[slot] + pairbuf[m % N_PAIR]

        @pl.when(role == 0)
        def _():
            for s in range(SUB):
                hop_a(m, s, on_line(1)).start()

        @pl.when(role == 3)
        def _():
            for s in range(SUB):
                hop_a(m, s, on_line(2)).start()

    def stage_m(m):
        @pl.when(role == 2)
        def _():
            slot = m % N_HOP
            for s in range(SUB):
                hop_a(m, s, on_line(3)).wait_recv()
                hbuf[slot, sub(s)] = hbuf[slot, sub(s)] + rbuf_a[slot, sub(s)]
                hop_b(m, s, on_line(1)).start()

    def stage_o(m):
        @pl.when(role == 1)
        def _():
            slot = m % N_HOP
            for s in range(SUB):
                hop_a(m, s, on_line(0)).wait_recv()
                hop_b(m, s, on_line(2)).wait_recv()
                tbuf[m % N_TOT, sub(s)] = rbuf_a[slot, sub(s)] + hbuf[slot, sub(s)] + rbuf_b[slot, sub(s)]
                tot_on(m, s, on_line(2)).start()
                tot_back(m, s, on_line(0)).start()

    def stage_t(m):
        @pl.when(role == 0)
        def _():
            for s in range(SUB):
                hop_a(m, s, on_line(1)).wait_send()
                tot_back(m, s, on_line(1)).wait_recv()

        @pl.when(role == 1)
        def _():
            for s in range(SUB):
                tot_back(m, s, on_line(0)).wait_send()
                tot_on(m, s, on_line(2)).wait_send()

        @pl.when(role == 2)
        def _():
            for s in range(SUB):
                hop_b(m, s, on_line(1)).wait_send()
                tot_on(m, s, on_line(1)).wait_recv()
                tot_on(m, s, on_line(3)).start()

        @pl.when(role == 3)
        def _():
            for s in range(SUB):
                hop_a(m, s, on_line(2)).wait_send()

    def stage_f1(m):
        for s in range(SUB):
            @pl.when(role == 3)
            def _(s=s):
                tot_on(m, s, on_line(2)).wait_recv()

            half_copy(m, s).start()

    def stage_f2(m):
        @pl.when(role == 2)
        def _():
            for s in range(SUB):
                tot_on(m, s, on_line(3)).wait_send()

        own = pl.ds(pl.multiple_of(core * half, PAIR), half)
        other = pl.ds(pl.multiple_of((1 - core) * half, PAIR), half)
        for s in range(SUB):
            half_copy(m, s).wait()
            rows = pl.ds(pl.multiple_of((m % n_chunks) * CHUNK + s * SUB_ROWS, SUB_ROWS), SUB_ROWS)
            cur[rows, own] = (cur[rows, own].astype(F32) + tbuf[m % N_TOT, sub(s)]).astype(BF16)
            cur[rows, other] = (cur[rows, other].astype(F32) + halfbuf[m % N_PAIR, sub(s)]).astype(BF16)

    def step(i, carry):
        for lag, stage in ((LAG_F2, stage_f2), (LAG_F1, stage_f1), (LAG_T, stage_t), (LAG_O, stage_o), (LAG_M, stage_m), (LAG_H, stage_h), (LAG_B, stage_b)):
            k = i - lag
            item = jnp.where(k >= EARLY_ONE, k, jnp.where(k >= EARLY_TWO - 1, k + 1, k + 2))
            steady = jnp.logical_and(k >= EARLY_ONE, k < n_items)
            one_early = jnp.logical_and(k + 1 >= EARLY_TWO, k + 1 < EARLY_ONE)
            two_early = jnp.logical_and(k + 2 >= 0, k + 2 < EARLY_TWO)

            @pl.when(jnp.logical_or(steady, jnp.logical_or(one_early, two_early)))
            def _(item=item, stage=stage):
                stage(item)

        @pl.when(i < n_items)
        def _():
            stage_a(i)
        return carry

    stage_a(jnp.int32(0), lambda: pl.semaphore_wait(barrier, tp - 1))
    lax.fori_loop(1, n_items + LAG_F2, step, 0)


def write_out(cur, out, sem):
    n_parts = sem.shape[0]
    rows = cur.shape[0] // n_parts
    copies = [pltpu.make_async_copy(cur.at[pl.ds(k * rows, rows)], out.at[pl.ds(k * rows, rows)], sem.at[k]) for k in range(n_parts)]
    for copy in copies:
        copy.start()
    for copy in copies:
        copy.wait()


def solution(mesh):
    tp = mesh.shape['tp']
    rep_spec = P()
    col_spec = P(None, None, 'tp')
    vec_spec = P(None, 'tp')
    in_specs = (P('dp'), rep_spec, col_spec, col_spec, rep_spec, col_spec, col_spec, rep_spec, vec_spec, rep_spec, vec_spec, vec_spec, vec_spec, vec_spec, P(None, 'tp', None))

    def device_forward(hidden, norm_w, w_z, w_x, w_bc, w_dt, conv_x, conv_bc, bias_x, bias_bc, dt_bias, a_log, d_skip, gate_w, w_out):
        n_layers, d_model, width = w_z.shape
        n_steps = hidden.shape[1]
        n_chunks = n_steps // CHUNK
        bc_width = w_bc.shape[-1]
        half = d_model // 2
        small = (norm_w, jnp.transpose(w_dt, (2, 0, 1)), conv_x, conv_bc, bias_x, bias_bc, dt_bias, a_log, d_skip, gate_w)
        hbm_spec = pl.BlockSpec(memory_space=pltpu.HBM)
        vmem_spec = pl.BlockSpec(memory_space=pltpu.VMEM)
        dma = pltpu.SemaphoreType.DMA
        block = (CHUNK, half)
        out = pl.pallas_call(
            functools.partial(kernel, n_chunks, n_layers, tp, width * tp),
            out_shape=pltpu.VMEM((n_steps, d_model), BF16),
            in_specs=[hbm_spec] * (5 + len(small)),
            out_specs=vmem_spec,
            scratch_shapes=[
                pltpu.VMEM((n_layers, d_model, width), BF16),
                pltpu.VMEM((n_layers, d_model, width), BF16),
                pltpu.VMEM((n_layers, d_model, bc_width), BF16),
                pltpu.VMEM((n_layers, PAIR, d_model), BF16),
                pltpu.VMEM((16, d_model), F32),
                pltpu.VMEM((n_layers, 2, width, half), BF16),
                pltpu.VMEM((n_layers, 16, d_model), F32),
                pltpu.VMEM((CHUNK + 8, width + bc_width), F32),
                pltpu.VMEM((bc_width // 2, width), F32),
                pltpu.VMEM((N_V, CHUNK, width), F32),
                pltpu.VMEM((N_STAT, tp, 1, CHUNK), F32),
                pltpu.VMEM((N_PAIR,) + block, F32),
                pltpu.VMEM((N_PAIR,) + block, F32),
                pltpu.VMEM((N_HOP,) + block, F32),
                pltpu.VMEM((N_HOP,) + block, F32),
                pltpu.VMEM((N_HOP,) + block, F32),
                pltpu.VMEM((N_TOT,) + block, F32),
                pltpu.VMEM((N_PAIR,) + block, F32),
                *[pltpu.VMEM(v.shape, v.dtype) for v in small],
                dma((n_chunks,)), dma((n_layers, 5)), dma((len(small),)),
                dma((N_STAT, tp)), dma((N_STAT, tp)), dma((N_PAIR,)), dma((N_PAIR,)),
                dma((N_HOP, SUB)), dma((N_HOP, SUB)), dma((N_HOP, SUB)),
                dma((N_TOT, SUB)), dma((N_TOT, SUB)), dma((N_TOT, SUB)), dma((N_PAIR, SUB)), dma((N_PAIR, SUB)),
            ],
            compiler_params=pltpu.CompilerParams(collective_id=0, has_side_effects=True, vmem_limit_bytes=VMEM_BYTES - 2 * n_steps * d_model),
        )(hidden.reshape(n_steps, d_model), w_z, w_x, w_bc, w_out, *small)
        out = pl.pallas_call(
            write_out,
            out_shape=jax.ShapeDtypeStruct((n_steps, d_model), BF16),
            in_specs=[vmem_spec],
            out_specs=hbm_spec,
            scratch_shapes=[dma((8,))],
            compiler_params=pltpu.CompilerParams(vmem_limit_bytes=1024 * 1024),
        )(out)
        return out.reshape(1, n_steps, d_model)

    return jax.shard_map(device_forward, mesh=mesh, in_specs=in_specs, out_specs=P('dp'), check_vma=False)
```

```python
import functools

import jax
import jax.numpy as jnp
from jax import lax
from jax.experimental import pallas as pl
from jax.experimental.pallas import tpu as pltpu
from jax.sharding import PartitionSpec as P

EPSILON = 1e-5
CHUNK = 128
PAIR = 128
HEAD_DIM = 64
HIGHEST = lax.Precision.HIGHEST
F32 = jnp.float32
BF16 = jnp.bfloat16

LAG_B, LAG_H, LAG_M, LAG_O, LAG_T, LAG_F1, LAG_F2 = 3, 4, 6, 7, 9, 11, 12
N_V, N_STAT, N_PAIR, N_HOP, N_TOT = 4, 8, 4, 8, 16
EARLY_TWO, EARLY_ONE = 2, 5
SUB = 4
SUB_ROWS = CHUNK // SUB
AHEAD = 4
VMEM_BYTES = 67043328
ROW_CONV, ROW_BIAS, ROW_NORM, ROW_GATE, ROW_SKIP, ROW_DT, ROW_A = 0, 4, 5, 6, 7, 8, 9


def fdot(a, b):
    return jnp.dot(a, b, precision=HIGHEST, preferred_element_type=F32)


def bdot(a, b):
    return jnp.dot(a, b, preferred_element_type=F32)


def kernel(n_chunks, n_layers, tp, inner_width,
           hid, wz, wx, wbc, wo, small_0, small_1, small_2, small_3, small_4, small_5, small_6, small_7, small_8, small_9, cur,
           wzv, wxv, wbcv, wdtv, dt_rows, wov, par, conv_in, state, vbuf, stat,
           obuf, pairbuf, hbuf, rbuf_a, rbuf_b, tbuf, halfbuf,
           norm_w, wdt, conv_x, conv_bc, bias_x, bias_bc, dt_bias, a_log, d_skip, gate_w,
           hid_sem, w_sem, small_sem,
           stat_send, stat_recv, pair_send, pair_recv, hop_send, hop_recv_a, hop_recv_b,
           tot_send_l, tot_send_r, tot_recv, half_send, half_recv):
    n_items = n_chunks * n_layers
    half = cur.shape[1] // 2
    width = wz.shape[-1]
    bc_width = wbc.shape[-1]
    heads = dt_bias.shape[-1]
    n_pairs = width // PAIR
    n_chips = tp // 2
    me = lax.axis_index('tp')
    z = me // 2
    core = me % 2
    partner = z * 2 + (1 - core)
    role = z + core * (n_chips - 1 - 2 * z)

    def on_line(k):
        return (k + core * (n_chips - 1 - 2 * k)) * 2 + core

    def remote(src, dst, send, recv, device):
        return pltpu.make_async_remote_copy(src_ref=src, dst_ref=dst, send_sem=send, recv_sem=recv, device_id={'tp': device}, device_id_type=pl.DeviceIdType.MESH)

    def chunk_rows(c):
        return pl.ds(pl.multiple_of(c * CHUNK, CHUNK), CHUNK)

    def hid_copy(c):
        return pltpu.make_async_copy(hid.at[chunk_rows(c), :], cur.at[chunk_rows(c), :], hid_sem.at[c])

    def w_copies(l):
        return [
            pltpu.make_async_copy(wz.at[l], wzv.at[l], w_sem.at[l, 0]),
            pltpu.make_async_copy(wx.at[l], wxv.at[l], w_sem.at[l, 1]),
            pltpu.make_async_copy(wbc.at[l], wbcv.at[l], w_sem.at[l, 2]),
            pltpu.make_async_copy(wo.at[l, :, pl.ds(0, half)], wov.at[l, 0], w_sem.at[l, 3]),
            pltpu.make_async_copy(wo.at[l, :, pl.ds(half, half)], wov.at[l, 1], w_sem.at[l, 4]),
        ]

    sources = (small_0, small_1, small_2, small_3, small_4, small_5, small_6, small_7, small_8, small_9)
    small = [pltpu.make_async_copy(src, dst, small_sem.at[k]) for k, (src, dst) in enumerate(zip(sources, (norm_w, wdt, conv_x, conv_bc, bias_x, bias_bc, dt_bias, a_log, d_skip, gate_w)))]
    for copy in small:
        copy.start()
    hid_copy(0).start()
    for copy in w_copies(0):
        copy.start()
    for c in range(1, AHEAD):
        hid_copy(c).start()

    barrier = pltpu.get_barrier_semaphore()
    for d in range(1, tp):
        pl.semaphore_signal(barrier, inc=1, device_id={'tp': (me + d) % tp}, device_id_type=pl.DeviceIdType.MESH)

    par[...] = jnp.zeros_like(par)
    dt_rows[...] = jnp.zeros_like(dt_rows)
    wdtv[...] = jnp.zeros_like(wdtv)
    for copy in small:
        copy.wait()
    for l in range(n_layers):
        par[l, ROW_CONV:ROW_CONV + 4, 0:width] = conv_x[l].astype(F32)
        par[l, ROW_CONV:ROW_CONV + 4, width:width + bc_width] = conv_bc[l].astype(F32)
        par[l, ROW_BIAS:ROW_BIAS + 1, 0:width] = bias_x[...].astype(F32)[l:l + 1]
        par[l, ROW_BIAS:ROW_BIAS + 1, width:width + bc_width] = bias_bc[...].astype(F32)[l:l + 1]
        par[l, ROW_NORM:ROW_NORM + 1, :] = norm_w[...].astype(F32)[l:l + 1]
        par[l, ROW_GATE:ROW_GATE + 1, 0:width] = gate_w[...].astype(F32)[l:l + 1]
        par[l, ROW_SKIP:ROW_SKIP + 1, 0:heads] = d_skip[l:l + 1, :]
        par[l, ROW_DT:ROW_DT + 1, 0:heads] = dt_bias[l:l + 1, :]
        par[l, ROW_A:ROW_A + 1, 0:heads] = a_log[l:l + 1, :]
        for n in range(heads):
            dt_rows[n:n + 1, :] = wdt[n].astype(F32)[l:l + 1]
        wdtv[l, 0:dt_rows.shape[0], :] = dt_rows[...].astype(BF16)

    row_id = lax.broadcasted_iota(jnp.int32, (CHUNK, CHUNK), 0)
    col_id = lax.broadcasted_iota(jnp.int32, (CHUNK, CHUNK), 1)

    def stat_copy(m, d):
        slot = m % N_STAT
        return remote(stat.at[slot, me], stat.at[slot, me], stat_send.at[slot, d], stat_recv.at[slot, me], (me + d) % tp)

    def stat_arrival(m, d):
        slot = m % N_STAT
        peer = (me + d) % tp
        return remote(stat.at[slot, peer], stat.at[slot, peer], stat_send.at[slot, d], stat_recv.at[slot, peer], peer)

    def pair_copy(m):
        slot = m % N_PAIR
        return remote(obuf.at[slot], pairbuf.at[slot], pair_send.at[slot], pair_recv.at[slot], partner)

    def sub(s):
        return pl.ds(s * SUB_ROWS, SUB_ROWS)

    def hop_a(m, s, device):
        slot = m % N_HOP
        return remote(hbuf.at[slot, sub(s)], rbuf_a.at[slot, sub(s)], hop_send.at[slot, s], hop_recv_a.at[slot, s], device)

    def hop_b(m, s, device):
        slot = m % N_HOP
        return remote(hbuf.at[slot, sub(s)], rbuf_b.at[slot, sub(s)], hop_send.at[slot, s], hop_recv_b.at[slot, s], device)

    def tot_back(m, s, device):
        slot = m % N_TOT
        return remote(tbuf.at[slot, sub(s)], tbuf.at[slot, sub(s)], tot_send_l.at[slot, s], tot_recv.at[slot, s], device)

    def tot_on(m, s, device):
        slot = m % N_TOT
        return remote(tbuf.at[slot, sub(s)], tbuf.at[slot, sub(s)], tot_send_r.at[slot, s], tot_recv.at[slot, s], device)

    def half_copy(m, s):
        slot = m % N_PAIR
        return remote(tbuf.at[m % N_TOT, sub(s)], halfbuf.at[slot, sub(s)], half_send.at[slot, s], half_recv.at[slot, s], partner)

    def stage_a(m, before_send=None):
        l = m // n_chunks
        c = m % n_chunks

        @pl.when(l == 0)
        def _():
            hid_copy(c).wait()

        @pl.when(m + AHEAD < n_chunks)
        def _():
            hid_copy(m + AHEAD).start()

        for later in range(1, n_layers):
            @pl.when(m == later * AHEAD)
            def _(later=later):
                for copy in w_copies(later):
                    copy.start()

        @pl.when(c == 0)
        def _():
            for copy in w_copies(l):
                copy.wait()
            conv_in[0:8, :] = jnp.zeros((8, conv_in.shape[1]), F32)
            state[...] = jnp.zeros_like(state)

        rows = chunk_rows(c)
        u = cur[rows, :].astype(F32)
        scale = lax.rsqrt(jnp.mean(u * u, axis=-1, keepdims=True) + EPSILON)
        h = (u * scale * par[l, ROW_NORM:ROW_NORM + 1, :]).astype(BF16)
        gate_z = bdot(h, wzv[l]).astype(BF16).astype(F32)
        conv_in[8:8 + CHUNK, 0:width] = bdot(h, wxv[l]).astype(BF16).astype(F32)
        conv_in[8:8 + CHUNK, width:] = bdot(h, wbcv[l]).astype(BF16).astype(F32)
        dt_pre = lax.dot_general(h, wdtv[l], (((1,), (1,)), ((), ())), preferred_element_type=F32).astype(BF16).astype(F32)

        cw = conv_in.shape[1]
        conv = par[l, ROW_BIAS:ROW_BIAS + 1, 0:cw]
        for j in range(4):
            conv = conv + conv_in[5 + j:5 + j + CHUNK, :] * par[l, ROW_CONV + j:ROW_CONV + j + 1, 0:cw]
        act = conv * jax.nn.sigmoid(conv)
        conv_in[0:8, :] = conv_in[CHUNK:CHUNK + 8, :]
        n_state = (cw - width) // 2
        b_in = act[:, width:width + n_state]
        c_in = act[:, width + n_state:]

        pre = dt_pre + par[l, ROW_DT:ROW_DT + 1, 0:PAIR]
        dt = jnp.maximum(pre, 0.0) + jnp.log1p(jnp.exp(-jnp.abs(pre)))
        a = -dt * jnp.exp(par[l, ROW_A:ROW_A + 1, 0:PAIR])
        lower = row_id >= col_id
        a_cum = fdot(jnp.where(lower, 1.0, 0.0).astype(F32), a)
        a_cum_t = a_cum.T
        a_last = a_cum[CHUNK - 1:CHUNK, :]
        grow = jnp.exp(a_cum)
        tail = jnp.exp(a_last - a_cum)
        carry = jnp.exp(a_last)
        b_t = b_in.T
        s_in = state[...]
        from_c = fdot(c_in, jnp.concatenate([b_t, s_in], axis=1))
        c_dot_b = from_c[:, 0:CHUNK]
        first = lax.broadcasted_iota(jnp.int32, (1, PAIR), 1) < HEAD_DIM
        v_slot = m % N_V
        sq = jnp.zeros((CHUNK, PAIR), F32)
        x_tail, carries = [], []
        skip = par[l, ROW_SKIP:ROW_SKIP + 1, 0:PAIR]
        for p in range(n_pairs):
            lanes = slice(p * PAIR, (p + 1) * PAIR)

            def spread(q):
                return jnp.where(first, q[:, 2 * p:2 * p + 1], q[:, 2 * p + 1:2 * p + 2])

            def mix(n):
                seg = a_cum[:, n:n + 1] - a_cum_t[n:n + 1, :]
                return jnp.where(lower, jnp.exp(jnp.minimum(seg, 0.0)), 0.0) * c_dot_b

            x = act[:, lanes]
            x_dt = x * spread(dt)
            mixes = jnp.concatenate([mix(2 * p), mix(2 * p + 1)], axis=1)
            x_both = jnp.concatenate([jnp.where(first, x_dt, 0.0), jnp.where(first, 0.0, x_dt)], axis=0)
            y_in = fdot(mixes, x_both)
            y_st = from_c[:, CHUNK + p * PAIR:CHUNK + (p + 1) * PAIR] * spread(grow)
            x_tail.append(x_dt * spread(tail))
            carries.append(spread(carry))
            y = y_in + y_st + spread(skip) * x
            zp = gate_z[:, lanes]
            v = y * (zp * jax.nn.sigmoid(zp))
            vbuf[v_slot, :, lanes] = v
            sq = sq + v * v
        state[...] = s_in * jnp.concatenate(carries, axis=1) + fdot(b_t, jnp.concatenate(x_tail, axis=1))
        part = jnp.broadcast_to(jnp.sum(sq, axis=-1, keepdims=True), (CHUNK, PAIR)).T
        stat[m % N_STAT, me] = part[0:1, :]
        if before_send is not None:
            before_send()
        for d in range(1, tp):
            stat_copy(m, d).start()

    def stage_b(m):
        l = m // n_chunks
        for d in range(1, tp):
            stat_copy(m, d).wait_send()
            stat_arrival(m, d).wait_recv()
        slot = m % N_STAT
        total = stat[slot, 0]
        for s in range(1, tp):
            total = total + stat[slot, s]
        total = jnp.broadcast_to(total, (PAIR, CHUNK)).T
        scale = lax.rsqrt(total / inner_width + EPSILON)
        parts = []
        for p in range(n_pairs):
            lanes = slice(p * PAIR, (p + 1) * PAIR)
            parts.append((vbuf[m % N_V, :, lanes] * scale * par[l, ROW_GATE:ROW_GATE + 1, lanes]).astype(BF16))
        g = jnp.concatenate(parts, axis=1)
        obuf[m % N_PAIR] = bdot(g, wov[l, 1 - core])
        pair_copy(m).start()
        hbuf[m % N_HOP] = bdot(g, wov[l, core])

    def stage_h(m):
        pair_copy(m).wait()
        slot = m % N_HOP
        hbuf[slot] = hbuf[slot] + pairbuf[m % N_PAIR]

        @pl.when(role == 0)
        def _():
            for s in range(SUB):
                hop_a(m, s, on_line(1)).start()

        @pl.when(role == 3)
        def _():
            for s in range(SUB):
                hop_a(m, s, on_line(2)).start()

    def stage_m(m):
        @pl.when(role == 2)
        def _():
            slot = m % N_HOP
            for s in range(SUB):
                hop_a(m, s, on_line(3)).wait_recv()
                hbuf[slot, sub(s)] = hbuf[slot, sub(s)] + rbuf_a[slot, sub(s)]
                hop_b(m, s, on_line(1)).start()

    def stage_o(m):
        @pl.when(role == 1)
        def _():
            slot = m % N_HOP
            for s in range(SUB):
                hop_a(m, s, on_line(0)).wait_recv()
                hop_b(m, s, on_line(2)).wait_recv()
                tbuf[m % N_TOT, sub(s)] = rbuf_a[slot, sub(s)] + hbuf[slot, sub(s)] + rbuf_b[slot, sub(s)]
                tot_on(m, s, on_line(2)).start()
                tot_back(m, s, on_line(0)).start()

    def stage_t(m):
        @pl.when(role == 0)
        def _():
            for s in range(SUB):
                hop_a(m, s, on_line(1)).wait_send()
                tot_back(m, s, on_line(1)).wait_recv()

        @pl.when(role == 1)
        def _():
            for s in range(SUB):
                tot_back(m, s, on_line(0)).wait_send()
                tot_on(m, s, on_line(2)).wait_send()

        @pl.when(role == 2)
        def _():
            for s in range(SUB):
                hop_b(m, s, on_line(1)).wait_send()
                tot_on(m, s, on_line(1)).wait_recv()
                tot_on(m, s, on_line(3)).start()

        @pl.when(role == 3)
        def _():
            for s in range(SUB):
                hop_a(m, s, on_line(2)).wait_send()

    def stage_f1(m):
        for s in range(SUB):
            @pl.when(role == 3)
            def _(s=s):
                tot_on(m, s, on_line(2)).wait_recv()

            half_copy(m, s).start()

    def stage_f2(m):
        @pl.when(role == 2)
        def _():
            for s in range(SUB):
                tot_on(m, s, on_line(3)).wait_send()

        own = pl.ds(pl.multiple_of(core * half, PAIR), half)
        other = pl.ds(pl.multiple_of((1 - core) * half, PAIR), half)
        for s in range(SUB):
            half_copy(m, s).wait()
            rows = pl.ds(pl.multiple_of((m % n_chunks) * CHUNK + s * SUB_ROWS, SUB_ROWS), SUB_ROWS)
            cur[rows, own] = (cur[rows, own].astype(F32) + tbuf[m % N_TOT, sub(s)]).astype(BF16)
            cur[rows, other] = (cur[rows, other].astype(F32) + halfbuf[m % N_PAIR, sub(s)]).astype(BF16)

    def step(i, carry):
        for lag, stage in ((LAG_F2, stage_f2), (LAG_F1, stage_f1), (LAG_T, stage_t), (LAG_O, stage_o), (LAG_M, stage_m), (LAG_H, stage_h), (LAG_B, stage_b)):
            k = i - lag
            item = jnp.where(k >= EARLY_ONE, k, jnp.where(k >= EARLY_TWO - 1, k + 1, k + 2))
            steady = jnp.logical_and(k >= EARLY_ONE, k < n_items)
            one_early = jnp.logical_and(k + 1 >= EARLY_TWO, k + 1 < EARLY_ONE)
            two_early = jnp.logical_and(k + 2 >= 0, k + 2 < EARLY_TWO)

            @pl.when(jnp.logical_or(steady, jnp.logical_or(one_early, two_early)))
            def _(item=item, stage=stage):
                stage(item)

        @pl.when(i < n_items)
        def _():
            stage_a(i)
        return carry

    stage_a(jnp.int32(0), lambda: pl.semaphore_wait(barrier, tp - 1))
    lax.fori_loop(1, n_items + LAG_F2, step, 0)


def write_out(cur, out, sem):
    n_parts = sem.shape[0]
    rows = cur.shape[0] // n_parts
    copies = [pltpu.make_async_copy(cur.at[pl.ds(k * rows, rows)], out.at[pl.ds(k * rows, rows)], sem.at[k]) for k in range(n_parts)]
    for copy in copies:
        copy.start()
    for copy in copies:
        copy.wait()


def solution(mesh):
    tp = mesh.shape['tp']
    rep_spec = P()
    col_spec = P(None, None, 'tp')
    vec_spec = P(None, 'tp')
    in_specs = (P('dp'), rep_spec, col_spec, col_spec, rep_spec, col_spec, col_spec, rep_spec, vec_spec, rep_spec, vec_spec, vec_spec, vec_spec, vec_spec, P(None, 'tp', None))

    def device_forward(hidden, norm_w, w_z, w_x, w_bc, w_dt, conv_x, conv_bc, bias_x, bias_bc, dt_bias, a_log, d_skip, gate_w, w_out):
        n_layers, d_model, width = w_z.shape
        n_steps = hidden.shape[1]
        n_chunks = n_steps // CHUNK
        bc_width = w_bc.shape[-1]
        half = d_model // 2
        small = (norm_w, jnp.transpose(w_dt, (2, 0, 1)), conv_x, conv_bc, bias_x, bias_bc, dt_bias, a_log, d_skip, gate_w)
        hbm_spec = pl.BlockSpec(memory_space=pltpu.HBM)
        vmem_spec = pl.BlockSpec(memory_space=pltpu.VMEM)
        dma = pltpu.SemaphoreType.DMA
        block = (CHUNK, half)
        out = pl.pallas_call(
            functools.partial(kernel, n_chunks, n_layers, tp, width * tp),
            out_shape=pltpu.VMEM((n_steps, d_model), BF16),
            in_specs=[hbm_spec] * (5 + len(small)),
            out_specs=vmem_spec,
            scratch_shapes=[
                pltpu.VMEM((n_layers, d_model, width), BF16),
                pltpu.VMEM((n_layers, d_model, width), BF16),
                pltpu.VMEM((n_layers, d_model, bc_width), BF16),
                pltpu.VMEM((n_layers, PAIR, d_model), BF16),
                pltpu.VMEM((16, d_model), F32),
                pltpu.VMEM((n_layers, 2, width, half), BF16),
                pltpu.VMEM((n_layers, 16, d_model), F32),
                pltpu.VMEM((CHUNK + 8, width + bc_width), F32),
                pltpu.VMEM((bc_width // 2, width), F32),
                pltpu.VMEM((N_V, CHUNK, width), F32),
                pltpu.VMEM((N_STAT, tp, 1, CHUNK), F32),
                pltpu.VMEM((N_PAIR,) + block, F32),
                pltpu.VMEM((N_PAIR,) + block, F32),
                pltpu.VMEM((N_HOP,) + block, F32),
                pltpu.VMEM((N_HOP,) + block, F32),
                pltpu.VMEM((N_HOP,) + block, F32),
                pltpu.VMEM((N_TOT,) + block, F32),
                pltpu.VMEM((N_PAIR,) + block, F32),
                *[pltpu.VMEM(v.shape, v.dtype) for v in small],
                dma((n_chunks,)), dma((n_layers, 5)), dma((len(small),)),
                dma((N_STAT, tp)), dma((N_STAT, tp)), dma((N_PAIR,)), dma((N_PAIR,)),
                dma((N_HOP, SUB)), dma((N_HOP, SUB)), dma((N_HOP, SUB)),
                dma((N_TOT, SUB)), dma((N_TOT, SUB)), dma((N_TOT, SUB)), dma((N_PAIR, SUB)), dma((N_PAIR, SUB)),
            ],
            compiler_params=pltpu.CompilerParams(collective_id=0, has_side_effects=True, vmem_limit_bytes=VMEM_BYTES - 2 * n_steps * d_model),
        )(hidden.reshape(n_steps, d_model), w_z, w_x, w_bc, w_out, *small)
        out = pl.pallas_call(
            write_out,
            out_shape=jax.ShapeDtypeStruct((n_steps, d_model), BF16),
            in_specs=[vmem_spec],
            out_specs=hbm_spec,
            scratch_shapes=[dma((8,))],
            compiler_params=pltpu.CompilerParams(vmem_limit_bytes=1024 * 1024),
        )(out)
        return out.reshape(1, n_steps, d_model)

    return jax.shard_map(device_forward, mesh=mesh, in_specs=in_specs, out_specs=P('dp'), check_vma=False)
```
